512 devices in a mesh: freq: 8 (over z), tile: 64 (over y, x, core).
Axes of the slice: x: 4, y: 8, z: 8, core: 2. Of those that a mesh axis runs over, the one named last changes fastest.
Arguments:
- left_factor: bfloat16 [16, 8192, 32, 128], P('freq', 'tile'), may hold values from -0.09375 to 0.09375
- right_factor: bfloat16 [16, 8192, 32, 128], P('freq', 'tile'), may hold values from -0.25 to 0.25
- tile_ranks: int32 [16, 32, 32], P('freq'), may hold values from 16 to 64, as said below
- freq_order: int32 [16], replicated, may hold values from 0 to 15, each once
- mute_window: int32 [8192, 64], P(('tile', 'freq')), may hold values from 2 to 31
- direct_wave: float32 [16, 2, 8192, 64], P('freq', None, 'tile'), may hold values from -6 to 6
Outputs:
- focusing_plus: float32 [16, 2, 8192, 64], P('freq', None, 'tile')
- focusing_minus: float32 [16, 2, 8192, 64], P('freq', None, 'tile')
The draws below stay inside these ranges and needn't reach their ends.
Inputs may be any that keep to these rules, and one draw needn't show every extreme that they name: tile_ranks[m, i, j] is the rank of tile (i, j) in slot m; every slot has a tile of rank 64. `freq_order`: each frequency index appears in one slot.
All inputs are finite; a program needn't handle non-finite values.
Results may differ from the reference program's by a relative error of at most 0.0051.
Values may be sent and summed in bfloat16 or wider, within the bound.
A program may use at most 64 MiB of HBM per device.

```python
import math
import jax
import jax.numpy as jnp
from jax import lax

RECEIVERS = 8192
TILE = 256
RANK_MAX = 64
PANEL = 128
FREQS = 16
FOCAL = 64
ITERS = 1
SAMPLES = 32
BLOCKS = 32


def draw_tile_ranks(key, part):
    first_key, second_key = jax.random.split(key)
    ranks = jax.random.randint(first_key, (FREQS, BLOCKS, BLOCKS), RANK_MAX // 4, RANK_MAX + 1)
    chosen = jax.random.randint(second_key, (FREQS, 1, 1), 0, BLOCKS * BLOCKS)
    places = lax.broadcasted_iota(jnp.int32, (FREQS, BLOCKS, BLOCKS), 1) * BLOCKS + lax.broadcasted_iota(jnp.int32, (FREQS, BLOCKS, BLOCKS), 2)
    return jnp.where(places == chosen, RANK_MAX, ranks).astype(jnp.int32)


def set_ends(array, stream_key, least, largest):
    longest = array.shape.index(max(array.shape))
    spots = []
    for shift in (0, 1):
        where = [jax.random.randint(jax.random.fold_in(stream_key, axis), (), 0, length) for axis, length in enumerate(array.shape)]
        where[longest] = (where[longest] + shift) % array.shape[longest]
        spots.append(tuple(where))
    return array.at[spots[0]].set(least).at[spots[1]].set(largest)


def level_of(rng, extent, cuts, least, largest):
    level = 1.0
    for position, blocks in cuts:
        heights = jax.random.uniform(jax.random.fold_in(jax.random.fold_in(rng, 6), position), (blocks,), jnp.float32, least / len(cuts), largest / len(cuts))
        level = level * jnp.repeat(jnp.exp(heights), extent[position] // blocks).reshape((-1,) + (1,) * (len(extent) - 1 - position))
    return level


def noise(rng, dims, width, bound, cuts=(), kind=jnp.bfloat16):
    values = jax.random.normal(rng, dims, jnp.float32) * width
    if len(cuts) > 0:
        values = level_of(rng, dims, cuts, -0.22, 0.18) * values
    return jnp.clip(values, min=-bound, max=bound).astype(kind)


def setup_inputs(seed: int = 0) -> dict:
    splits = jax.random.split(jax.random.key(seed), 7)
    left_factor = noise(splits[0], (FREQS, RECEIVERS, BLOCKS, 2 * RANK_MAX), (2 * BLOCKS * RANK_MAX) ** -0.5, 0.09375, ((0, 8), (1, 64)))
    right_factor = noise(splits[1], (FREQS, RECEIVERS, BLOCKS, 2 * RANK_MAX), (2 * TILE) ** -0.5, 0.25, ((0, 8), (1, 64)))
    tile_ranks = draw_tile_ranks(jax.random.fold_in(splits[6], 71), 0)
    freq_order = jax.random.permutation(splits[3], FREQS).astype(jnp.int32)
    mute_window = set_ends(jax.random.randint(splits[4], (RECEIVERS, FOCAL), 2, SAMPLES), jax.random.fold_in(splits[4], 1), 2, SAMPLES - 1).astype(jnp.int32)
    direct_wave = noise(splits[5], (FREQS, 2, RECEIVERS, FOCAL), 1.0, 6.0, ((0, 8), (2, 64)), jnp.float32)
    return {"left_factor": left_factor, "right_factor": right_factor, "tile_ranks": tile_ranks, "freq_order": freq_order, "mute_window": mute_window, "direct_wave": direct_wave}


def transform_tables(freq_order):
    angular = (freq_order.astype(jnp.float32) + 0.5) * (2.0 * math.pi / SAMPLES)
    sample_times = jnp.arange(SAMPLES, dtype=jnp.float32)
    phases = sample_times[:, None] * angular[None, :]
    columns = jnp.stack([jnp.cos(phases), -jnp.sin(phases)], axis=2).reshape(SAMPLES, 2 * FREQS)
    return columns * (2.0 / SAMPLES), columns.T


def combine(products, signum):
    rank_most = products.shape[-2] // 2
    focal_count = products.shape[-1] // 2
    real_real = products[..., :rank_most, :focal_count]
    real_imag = products[..., :rank_most, focal_count:]
    imag_real = products[..., rank_most:, :focal_count]
    imag_imag = products[..., rank_most:, focal_count:]
    return jnp.concatenate([real_real - signum * imag_imag, real_imag + signum * imag_real], axis=-1)


def apply_kernel(inner_factor, outer_factor, ranks_oriented, signum, fields):
    def one_slot(operands):
        inner_slot, outer_slot, rank_slot, field_slot = operands
        joined = jnp.concatenate([field_slot[0], field_slot[1]], axis=1).astype(jnp.bfloat16)
        joined = lax.optimization_barrier(joined).astype(jnp.float32)
        panels = inner_slot.astype(jnp.float32).reshape(RECEIVERS // PANEL, PANEL, BLOCKS, 2 * RANK_MAX)
        products = jnp.einsum("gbik,gbq->igkq", panels, joined.reshape(RECEIVERS // PANEL, PANEL, 2 * FOCAL), precision=lax.Precision.HIGHEST)
        rounded = lax.optimization_barrier(combine(products, signum).astype(jnp.bfloat16)).astype(jnp.float32)
        summed = rounded.reshape(BLOCKS, BLOCKS, TILE // PANEL, RANK_MAX, 2 * FOCAL).sum(axis=2)
        within = jnp.arange(RANK_MAX)[None, None, :, None] < rank_slot[:, :, None, None]
        coefficients = jnp.where(within, summed, 0.0).astype(jnp.bfloat16)
        second_half = jnp.concatenate([-signum * coefficients[..., FOCAL:], signum * coefficients[..., :FOCAL]], axis=-1)
        stacked = jnp.concatenate([coefficients, second_half], axis=2).astype(jnp.float32)
        outer_blocks = outer_slot.astype(jnp.float32).reshape(BLOCKS, TILE, BLOCKS, 2 * RANK_MAX)
        result = jnp.einsum("ibjk,ijkq->ibq", outer_blocks, stacked, precision=lax.Precision.HIGHEST).reshape(RECEIVERS, 2 * FOCAL)
        return jnp.stack([result[:, :FOCAL], result[:, FOCAL:]], axis=0)

    return lax.map(one_slot, (inner_factor, outer_factor, ranks_oriented, fields))


def mute(spectra, mute_window, inverse, forward):
    stacked = spectra.reshape(2 * FREQS, RECEIVERS * FOCAL)
    in_time = jnp.dot(inverse, stacked, precision=lax.Precision.HIGHEST)
    kept_mask = jnp.arange(SAMPLES)[:, None] < mute_window.reshape(1, RECEIVERS * FOCAL)
    muted = jnp.where(kept_mask, in_time, 0.0)
    return jnp.dot(forward, muted, precision=lax.Precision.HIGHEST).reshape(FREQS, 2, RECEIVERS, FOCAL)


def reference(left_factor, right_factor, tile_ranks, freq_order, mute_window, direct_wave):
    inverse, forward = transform_tables(freq_order)
    swapped = jnp.swapaxes(tile_ranks, 1, 2)
    focus_plus = direct_wave
    focus_minus = direct_wave
    for iteration in range(ITERS):
        focus_minus = mute(apply_kernel(right_factor, left_factor, tile_ranks, 1.0, focus_plus), mute_window, inverse, forward)
        focus_plus = direct_wave + mute(apply_kernel(left_factor, right_factor, swapped, -1.0, focus_minus), mute_window, inverse, forward)
    return focus_plus, focus_minus
```

```python
import functools
import math

import jax
import jax.numpy as jnp
from jax import lax
from jax.experimental import pallas as pl
from jax.experimental.pallas import tpu as pltpu
from jax.sharding import PartitionSpec as P

GRID = {64: (8, 4), 8: (2, 2)}
PITCH = 40
ROWS = 128
LANES = 128
HALF = 64
MESH = pl.DeviceIdType.MESH


def roll_half(value):
    return jnp.concatenate([value[:, HALF:], value[:, :HALF]], axis=1)


def kernel(
    dims,
    right_hbm,
    left_hbm,
    ranks_hbm,
    order_hbm,
    window_hbm,
    direct_hbm,
    plus_hbm,
    minus_hbm,
    raw,
    spread,
    right_all,
    left_all,
    right_out,
    left_out,
    direct,
    window,
    ranks,
    order,
    joined,
    joined_out,
    partial,
    sent_a,
    sent_b,
    got_a,
    got_b,
    total,
    image_a,
    image_b,
    gathered_a,
    gathered_b,
    weights,
    samples,
    muted_a,
    muted_b,
    focus,
    swap_out,
    swap_in,
    final,
    minus_stage,
    plus_stage,
    raw_sem,
    in_sem,
    out_sem,
    pair_send,
    pair_recv,
    right_send,
    right_recv,
    left_send,
    left_recv,
    tile_send_a,
    tile_recv_a,
    tile_send_b,
    tile_recv_b,
    freq_send_a,
    freq_recv_a,
    freq_send_b,
    freq_recv_b,
    back_send_a,
    back_recv_a,
    back_send_b,
    back_recv_b,
):
    ny, nx, nz, samples_count = dims
    blocks = ny * nx
    slots = 2 * nz
    rows_each = ROWS // nz
    depth = lax.axis_index("freq")
    tile = lax.axis_index("tile")
    core = lax.rem(tile, 2)
    other = 1 - core
    chip = tile // 2
    chip_y = chip // nx
    chip_x = lax.rem(chip, nx)

    def to_tile(index):
        return {"freq": depth, "tile": index}

    def local(source, target, sem):
        return pltpu.make_async_copy(source, target, sem)

    def remote(source, target, send, recv, device):
        return pltpu.make_async_remote_copy(
            src_ref=source,
            dst_ref=target,
            send_sem=send,
            recv_sem=recv,
            device_id=device,
            device_id_type=MESH,
        )

    partner = {"freq": depth, "tile": tile + other - core}

    small = [
        local(direct_hbm, direct, in_sem.at[0]),
        local(window_hbm, window, in_sem.at[1]),
        local(ranks_hbm, ranks, in_sem.at[2]),
        local(order_hbm, order, in_sem.at[3]),
    ]
    raws = [
        local(right_hbm.at[0], raw.at[0], raw_sem.at[0]),
        local(right_hbm.at[1], raw.at[1], raw_sem.at[1]),
        local(left_hbm.at[0], raw.at[2], raw_sem.at[2]),
        local(left_hbm.at[1], raw.at[3], raw_sem.at[3]),
    ]
    for copy in small[:1] + raws[:2] + small[1:] + raws[2:]:
        copy.start()

    barrier = pltpu.get_barrier_semaphore()

    def greet_tile(index, carry):
        @pl.when(index != chip)
        def _():
            pl.semaphore_signal(
                barrier, inc=1, device_id=to_tile(index * 2 + core), device_id_type=MESH
            )

        return carry

    def greet_freq(index, carry):
        @pl.when(jnp.logical_or(index // 2 != depth, lax.rem(index, 2) != core))
        def _():
            pl.semaphore_signal(
                barrier,
                inc=1,
                device_id={"freq": index // 2, "tile": chip * 2 + lax.rem(index, 2)},
                device_id_type=MESH,
            )

        return carry

    lax.fori_loop(0, blocks, greet_tile, 0)
    lax.fori_loop(0, slots, greet_freq, 0)

    def reorder(slot, target):
        def widen(row, carry):
            for step in range(4):
                spread[pl.ds((row * 4 + step) * PITCH, blocks), :] = raw[
                    slot, row * 4 + step
                ].astype(jnp.float32)
            return carry

        lax.fori_loop(0, ROWS // 4, widen, 0)

        def narrow(index, carry):
            target[index] = spread[pl.ds(index, ROWS, stride=PITCH), :].astype(jnp.bfloat16)
            return carry

        lax.fori_loop(0, blocks, narrow, 0)

    small[0].wait()
    joined_out[...] = jnp.concatenate([direct[other, 0], direct[other, 1]], axis=0).astype(
        jnp.bfloat16
    )
    joined[core] = jnp.concatenate([direct[core, 0], direct[core, 1]], axis=0).astype(jnp.bfloat16)
    raws[0].wait()
    raws[1].wait()
    reorder(other, right_out)
    reorder(core, right_all.at[core])

    lane = lax.broadcasted_iota(jnp.int32, (HALF, LANES), 1)
    low = lane < HALF
    column = lax.rem(lane, HALF)

    def products(fields, factors, side, first, signum):
        wide = jnp.concatenate([factors[side, first + step] for step in range(nx)], axis=1)
        result = jnp.dot(fields, wide, preferred_element_type=jnp.float32)
        pieces = []
        for step in range(nx):
            real = result[:HALF, step * LANES : (step + 1) * LANES]
            turned = roll_half(result[HALF:, step * LANES : (step + 1) * LANES])
            if signum > 0:
                piece = jnp.where(low, real - turned, turned + real)
            else:
                piece = jnp.where(low, real + turned, turned - real)
            pieces.append(piece.astype(jnp.bfloat16))
        return pieces

    def row_of(step, sign):
        reach = ny // 2 - (step + 1) // 2
        offset = jnp.where(lax.rem(step, 2) == 1, reach, ny - reach)
        return lax.rem(chip_y + ny + sign * offset, ny)

    own_fields = joined[core]

    def own_group(step, carry):
        first = step * nx
        pieces = products(own_fields, right_all, core, first, 1.0)
        for index in range(nx):
            partial[first + index] = pieces[index]
        return carry

    lax.fori_loop(0, ny, own_group, 0)

    pl.semaphore_wait(barrier, blocks - 1 + slots - 1)

    pair = remote(joined_out, joined.at[core], pair_send.at[0], pair_recv.at[0], partner)
    pair.start()

    def factor_copy(step, source, target, send, recv):
        first = row_of(step, 1) * nx
        return remote(
            source.at[pl.ds(first, nx)],
            target.at[core, pl.ds(first, nx)],
            send.at[step],
            recv.at[step],
            partner,
        )

    def start_right(step, carry):
        factor_copy(step, right_out, right_all, right_send, right_recv).start()
        return carry

    lax.fori_loop(0, ny, start_right, 0)
    for copy in small[1:]:
        copy.wait()
    pair_in = remote(joined_out, joined.at[other], pair_send.at[0], pair_recv.at[0], partner)
    pair_in.wait_recv()

    def tile_copy(block, source, target, send, recv):
        return remote(
            source.at[block],
            target.at[chip],
            send.at[block],
            recv.at[chip],
            to_tile(block * 2 + core),
        )

    def emit(first, pieces, sent, got, send, recv, rank_of):
        for index in range(nx):
            block = first + index
            kept = jnp.where(column < rank_of(block), pieces[index], 0.0).astype(jnp.bfloat16)
            sent[block] = kept

            @pl.when(block == chip)
            def _():
                got[chip] = kept

        for index in range(nx):
            block = first + index

            @pl.when(block != chip)
            def _():
                tile_copy(block, sent, got, send, recv).start()

    def forward_group(step, carry):
        first = row_of(step, 1) * nx
        remote(
            right_out.at[pl.ds(first, nx)],
            right_all.at[other, pl.ds(first, nx)],
            right_send.at[step],
            right_recv.at[step],
            partner,
        ).wait_recv()
        pieces = products(joined[other], right_all, other, first, 1.0)
        summed = [
            pieces[index].astype(jnp.float32) + partial[first + index].astype(jnp.float32)
            for index in range(nx)
        ]
        emit(
            first,
            summed,
            sent_a,
            got_a,
            tile_send_a,
            tile_recv_a,
            lambda block: ranks[core, block, chip],
        )
        return carry

    lax.fori_loop(0, ny, forward_group, 0)

    raws[2].wait()
    raws[3].wait()
    reorder(2 + other, left_out)

    def start_left(step, carry):
        factor_copy(step, left_out, left_all, left_send, left_recv).start()
        return carry

    lax.fori_loop(0, ny, start_left, 0)
    reorder(2 + core, left_all.at[core])

    turn = 2 * samples_count
    moment = lax.broadcasted_iota(jnp.int32, (samples_count, LANES), 0)
    shift = jnp.where(
        lax.broadcasted_iota(jnp.int32, (samples_count, LANES), 1) < HALF, 0, samples_count // 2
    )

    def weight(slot, carry):
        phase = lax.rem(moment * (2 * order[slot] + 1) + shift, turn)
        weights[slot] = jnp.cos(phase.astype(jnp.float32) * (2.0 * math.pi / turn))
        return carry

    lax.fori_loop(0, slots, weight, 0)

    def wait_left(step, carry):
        first = row_of(step, 1) * nx
        remote(
            left_out.at[pl.ds(first, nx)],
            left_all.at[other, pl.ds(first, nx)],
            left_send.at[step],
            left_recv.at[step],
            partner,
        ).wait_recv()
        return carry

    lax.fori_loop(0, ny, wait_left, 0)

    side_low = lax.broadcasted_iota(jnp.int32, (HALF, LANES), 1) < HALF

    def finish(sent, got, send, recv, factors, signum):
        top_sign = jnp.where(side_low, 1.0, -signum)
        bottom_sign = jnp.where(side_low, 1.0, signum)

        def group(step, carry):
            first = row_of(step, -1) * nx
            for index in range(nx):
                block = first + index

                @pl.when(block != chip)
                def _():
                    remote(
                        sent.at[block],
                        got.at[block],
                        send.at[block],
                        recv.at[block],
                        partner,
                    ).wait_recv()

            columns = []
            for index in range(nx):
                piece = got[first + index].astype(jnp.float32)
                both = jnp.concatenate(
                    [piece * top_sign, roll_half(piece) * bottom_sign], axis=0
                )
                columns.append(both.astype(jnp.bfloat16))
            wide = jnp.concatenate(columns, axis=1)
            for side in range(2):
                rows = jnp.concatenate(
                    [factors[side, first + index] for index in range(nx)], axis=1
                )
                value = lax.dot_general(
                    rows, wide, (((1,), (1,)), ((), ())), preferred_element_type=jnp.float32
                )
                total[side] = total[side] + value
            return carry

        total[...] = jnp.zeros_like(total)
        lax.fori_loop(0, ny, group, 0)

    def to_owner(index, image, gathered, send, recv):
        return remote(
            image.at[index],
            gathered.at[2 * depth + core],
            send.at[index],
            recv.at[2 * depth + core],
            {"freq": lax.rem(index, nz), "tile": chip * 2 + index // nz},
        )

    def spread_image(image, gathered, send, recv):
        image[...] = total[...].reshape(slots, rows_each, LANES).astype(jnp.bfloat16)
        mine = core * nz + depth

        def one(step, carry):
            index = lax.rem(step // nz * nz + lax.rem(step + depth + nz // 2, nz), slots)

            @pl.when(index != mine)
            def _():
                to_owner(index, image, gathered, send, recv).start()

            return carry

        lax.fori_loop(0, slots, one, 0)
        gathered[2 * depth + core] = image[mine]

        def arrive(slot, carry):
            @pl.when(slot != 2 * depth + core)
            def _():
                remote(
                    image.at[0], gathered.at[slot], send.at[0], recv.at[slot], partner
                ).wait_recv()

            return carry

        lax.fori_loop(0, slots, arrive, 0)

    kept = jnp.concatenate([window[...], window[...]], axis=1)

    def mute(gathered, muted):
        values = [gathered[slot].astype(jnp.float32) for slot in range(slots)]

        def invert(step, carry):
            sums = values[0] * weights[0, pl.ds(step, 1), :]
            for slot in range(1, slots):
                sums = sums + values[slot] * weights[slot, pl.ds(step, 1), :]
            sums = (sums + roll_half(sums)) * (2.0 / samples_count)
            samples[step] = jnp.where(step < kept, sums, 0.0)
            return carry

        lax.fori_loop(0, samples_count, invert, 0)

        def forward(slot, carry):
            sums = samples[0] * weights[slot, pl.ds(0, 1), :]
            for step in range(1, samples_count):
                sums = sums + samples[step] * weights[slot, pl.ds(step, 1), :]
            muted[slot // 2, lax.rem(slot, 2)] = sums.astype(jnp.bfloat16)
            return carry

        lax.fori_loop(0, slots, forward, 0)

    finish(sent_a, got_a, tile_send_a, tile_recv_a, left_all, 1.0)
    spread_image(image_a, gathered_a, freq_send_a, freq_recv_a)
    mute(gathered_a, muted_a)

    def to_slot(level, side):
        return remote(
            muted_a.at[level, side],
            focus.at[core * nz + depth],
            back_send_a.at[level * 2 + side],
            back_recv_a.at[core * nz + depth],
            {"freq": level, "tile": chip * 2 + side},
        )

    def send_back(step, carry):
        level = lax.rem(step // 2 + depth + nz // 2, nz)
        side = lax.rem(step, 2)

        @pl.when(jnp.logical_or(level != depth, side != core))
        def _():
            to_slot(level, side).start()

        return carry

    lax.fori_loop(0, slots, send_back, 0)
    focus[core * nz + depth] = muted_a[depth, core]

    def wait_back(index, carry):
        @pl.when(index != core * nz + depth)
        def _():
            remote(
                muted_a.at[0, 0],
                focus.at[index],
                back_send_a.at[0],
                back_recv_a.at[index],
                partner,
            ).wait_recv()

        return carry

    lax.fori_loop(0, slots, wait_back, 0)

    turned = [
        focus[pl.ds(side * nz, nz)].reshape(ROWS, LANES).astype(jnp.float32).T for side in range(2)
    ]
    fields = [value.astype(jnp.bfloat16) for value in turned]

    def backward_group(step, carry):
        first = row_of(step, 1) * nx
        lower = products(fields[0], left_all, 0, first, -1.0)
        upper = products(fields[1], left_all, 1, first, -1.0)
        summed = [
            lower[index].astype(jnp.float32) + upper[index].astype(jnp.float32)
            for index in range(nx)
        ]
        emit(
            first,
            summed,
            sent_b,
            got_b,
            tile_send_b,
            tile_recv_b,
            lambda block: ranks[core, chip, block],
        )
        return carry

    lax.fori_loop(0, ny, backward_group, 0)

    swap_out[0] = fields[0]
    swap_out[1] = fields[1]
    swap = remote(swap_out.at[other], swap_in, pair_send.at[1], pair_recv.at[1], partner)
    swap.start()
    swap.wait_recv()
    own = swap_out[core].astype(jnp.float32)
    minus_stage[core, 0] = own[:HALF]
    minus_stage[core, 1] = own[HALF:]
    theirs = swap_in[...].astype(jnp.float32)
    minus_stage[other, 0] = theirs[:HALF]
    minus_stage[other, 1] = theirs[HALF:]
    minus_copy = local(minus_stage, minus_hbm, out_sem.at[0])
    minus_copy.start()

    finish(sent_b, got_b, tile_send_b, tile_recv_b, right_all, -1.0)
    spread_image(image_b, gathered_b, freq_send_b, freq_recv_b)
    mute(gathered_b, muted_b)

    def to_level(level):
        return remote(
            muted_b.at[level],
            final.at[depth],
            back_send_b.at[level],
            back_recv_b.at[depth],
            {"freq": level, "tile": tile},
        )

    def send_final(step, carry):
        level = lax.rem(step + depth + nz // 2, nz)

        @pl.when(level != depth)
        def _():
            to_level(level).start()

        return carry

    lax.fori_loop(0, nz, send_final, 0)
    final[depth] = muted_b[depth]

    def wait_final(index, carry):
        @pl.when(index != depth)
        def _():
            remote(
                muted_b.at[0],
                final.at[index],
                back_send_b.at[0],
                back_recv_b.at[index],
                partner,
            ).wait_recv()

        return carry

    lax.fori_loop(0, nz, wait_final, 0)
    for slot in range(2):
        value = final[:, slot].reshape(ROWS, LANES).astype(jnp.float32).T
        plus_stage[slot, 0] = direct[slot, 0] + value[:HALF]
        plus_stage[slot, 1] = direct[slot, 1] + value[HALF:]
    plus_copy = local(plus_stage, plus_hbm, out_sem.at[1])
    plus_copy.start()

    pair.wait_send()
    swap.wait_send()

    def drain_factors(step, carry):
        factor_copy(step, right_out, right_all, right_send, right_recv).wait_send()
        factor_copy(step, left_out, left_all, left_send, left_recv).wait_send()
        return carry

    lax.fori_loop(0, ny, drain_factors, 0)

    def drain_tiles(block, carry):
        @pl.when(block != chip)
        def _():
            tile_copy(block, sent_a, got_a, tile_send_a, tile_recv_a).wait_send()
            tile_copy(block, sent_b, got_b, tile_send_b, tile_recv_b).wait_send()

        return carry

    lax.fori_loop(0, blocks, drain_tiles, 0)

    def drain_freq(index, carry):
        @pl.when(index != core * nz + depth)
        def _():
            to_owner(index, image_a, gathered_a, freq_send_a, freq_recv_a).wait_send()
            to_owner(index, image_b, gathered_b, freq_send_b, freq_recv_b).wait_send()

        return carry

    lax.fori_loop(0, slots, drain_freq, 0)

    def drain_back(index, carry):
        level = index // 2
        side = lax.rem(index, 2)

        @pl.when(jnp.logical_or(level != depth, side != core))
        def _():
            to_slot(level, side).wait_send()

        return carry

    lax.fori_loop(0, slots, drain_back, 0)

    def drain_final(level, carry):
        @pl.when(level != depth)
        def _():
            to_level(level).wait_send()

        return carry

    lax.fori_loop(0, nz, drain_final, 0)
    minus_copy.wait()
    plus_copy.wait()


def shards(dims, left_factor, right_factor, tile_ranks, freq_order, mute_window, direct_wave):
    ny, nx, nz, samples_count = dims
    blocks = ny * nx
    slots = 2 * nz
    rows_each = ROWS // nz
    bf16, f32 = jnp.bfloat16, jnp.float32
    dma = pltpu.SemaphoreType.DMA
    turned = jnp.transpose(direct_wave, (0, 1, 3, 2))
    factor = (2, blocks, ROWS, LANES)
    tiles = (blocks, HALF, LANES)
    pieces = (slots, rows_each, LANES)
    stage = (2, 2, HALF, ROWS)
    scratch = [
        pltpu.VMEM((4, ROWS, blocks, LANES), bf16),
        pltpu.VMEM((ROWS * PITCH, LANES), f32),
        pltpu.VMEM(factor, bf16),
        pltpu.VMEM(factor, bf16),
        pltpu.VMEM(factor[1:], bf16),
        pltpu.VMEM(factor[1:], bf16),
        pltpu.VMEM(stage, f32),
        pltpu.VMEM(mute_window.shape, jnp.int32),
        pltpu.SMEM(tile_ranks.shape, jnp.int32),
        pltpu.SMEM(freq_order.shape, jnp.int32),
        pltpu.VMEM((2, LANES, ROWS), bf16),
        pltpu.VMEM((LANES, ROWS), bf16),
        pltpu.VMEM(tiles, bf16),
        pltpu.VMEM(tiles, bf16),
        pltpu.VMEM(tiles, bf16),
        pltpu.VMEM(tiles, bf16),
        pltpu.VMEM(tiles, bf16),
        pltpu.VMEM((2, ROWS, LANES), f32),
        pltpu.VMEM(pieces, bf16),
        pltpu.VMEM(pieces, bf16),
        pltpu.VMEM(pieces, bf16),
        pltpu.VMEM(pieces, bf16),
        pltpu.VMEM((slots, samples_count, LANES), f32),
        pltpu.VMEM((samples_count, rows_each, LANES), f32),
        pltpu.VMEM((nz, 2, rows_each, LANES), bf16),
        pltpu.VMEM((nz, 2, rows_each, LANES), bf16),
        pltpu.VMEM(pieces, bf16),
        pltpu.VMEM((2, LANES, ROWS), bf16),
        pltpu.VMEM((LANES, ROWS), bf16),
        pltpu.VMEM((nz, 2, rows_each, LANES), bf16),
        pltpu.VMEM(stage, f32),
        pltpu.VMEM(stage, f32),
        dma((4,)),
        dma((4,)),
        dma((2,)),
        dma((2,)),
        dma((2,)),
        dma((ny,)),
        dma((ny,)),
        dma((ny,)),
        dma((ny,)),
        dma((blocks,)),
        dma((blocks,)),
        dma((blocks,)),
        dma((blocks,)),
        dma((slots,)),
        dma((slots,)),
        dma((slots,)),
        dma((slots,)),
        dma((slots,)),
        dma((slots,)),
        dma((nz,)),
        dma((nz,)),
    ]
    out = jax.ShapeDtypeStruct(stage, f32)
    plus, minus = pl.pallas_call(
        functools.partial(kernel, dims),
        out_shape=(out, out),
        in_specs=[pl.BlockSpec(memory_space=pl.ANY)] * 6,
        out_specs=(pl.BlockSpec(memory_space=pl.ANY),) * 2,
        scratch_shapes=scratch,
        compiler_params=pltpu.CompilerParams(
            collective_id=0, has_side_effects=True, vmem_limit_bytes=48 * 1024 * 1024
        ),
        name="focusing",
    )(right_factor, left_factor, tile_ranks, freq_order, mute_window, turned)
    return jnp.transpose(plus, (0, 1, 3, 2)), jnp.transpose(minus, (0, 1, 3, 2))


def solution(mesh):
    nz = mesh.shape["freq"]
    ny, nx = GRID[mesh.shape["tile"]]
    dims = (ny, nx, nz, 4 * nz)
    return jax.shard_map(
        functools.partial(shards, dims),
        mesh=mesh,
        in_specs=(
            P("freq", "tile", None, None),
            P("freq", "tile", None, None),
            P("freq", None, None),
            P(),
            P(("tile", "freq"), None),
            P("freq", None, "tile", None),
        ),
        out_specs=(P("freq", None, "tile", None), P("freq", None, "tile", None)),
        check_vma=False,
    )
```

```python
import functools
import math

import jax
import jax.numpy as jnp
from jax import lax
from jax.experimental import pallas as pl
from jax.experimental.pallas import tpu as pltpu
from jax.sharding import PartitionSpec as P

GRID = {64: (8, 4), 8: (2, 2)}
PITCH = 40
CHUNKS = 2
FOCAL = 64
PART = FOCAL // CHUNKS
CHUNKS = 2
FOCAL = 64
PART = FOCAL // CHUNKS
CHUNKS = 2
FOCAL = 64
PART = FOCAL // CHUNKS
CHUNKS = 2
FOCAL = 64
PART = FOCAL // CHUNKS
ROWS = 128
LANES = 128
HALF = 64
MESH = pl.DeviceIdType.MESH


def roll_half(value):
    return pltpu.roll(value, HALF, 1)


def kernel(
    dims,
    right_hbm,
    left_hbm,
    ranks_hbm,
    order_hbm,
    window_hbm,
    direct_hbm,
    plus_hbm,
    minus_hbm,
    raw,
    spread,
    right_all,
    left_all,
    right_out,
    left_out,
    direct,
    window,
    limits,
    ranks,
    order,
    joined,
    joined_out,
    partial,
    sent,
    got,
    total,
    image,
    gathered,
    weights,
    samples,
    muted,
    focus,
    swap_out,
    swap_in,
    final,
    minus_stage,
    plus_stage,
    raw_sem,
    in_sem,
    out_sem,
    pair_send,
    pair_recv,
    swap_send,
    swap_recv,
    right_send,
    right_recv,
    left_send,
    left_recv,
    tile_send,
    tile_recv,
    freq_send,
    freq_recv,
    back_send,
    back_recv,
):
    ny, nx, nz, samples_count = dims
    blocks = ny * nx
    slots = 2 * nz
    rows_each = ROWS // nz
    steps = samples_count // CHUNKS
    depth = lax.axis_index("freq")
    tile = lax.axis_index("tile")
    core = lax.rem(tile, 2)
    other = 1 - core
    chip = tile // 2
    chip_y = chip // nx
    chip_x = lax.rem(chip, nx)
    partner = {"freq": depth, "tile": tile + other - core}
    mine = core * nz + depth
    slot_here = 2 * depth + core

    def local(source, target, sem):
        return pltpu.make_async_copy(source, target, sem)

    def remote(source, target, send, recv, device):
        return pltpu.make_async_remote_copy(
            src_ref=source,
            dst_ref=target,
            send_sem=send,
            recv_sem=recv,
            device_id=device,
            device_id_type=MESH,
        )

    small = [
        local(direct_hbm, direct, in_sem.at[0]),
        local(window_hbm, window, in_sem.at[1]),
        local(ranks_hbm, ranks, in_sem.at[2]),
        local(order_hbm, order, in_sem.at[3]),
    ]
    raws = [
        local(right_hbm.at[0], raw.at[0], raw_sem.at[0]),
        local(right_hbm.at[1], raw.at[1], raw_sem.at[1]),
        local(left_hbm.at[0], raw.at[2], raw_sem.at[2]),
        local(left_hbm.at[1], raw.at[3], raw_sem.at[3]),
    ]
    barrier = pltpu.get_barrier_semaphore()

    def greet_tile(index, carry):
        @pl.when(index != chip)
        def _():
            pl.semaphore_signal(
                barrier,
                inc=1,
                device_id={"freq": depth, "tile": index * 2 + core},
                device_id_type=MESH,
            )

        return carry

    def greet_freq(index, carry):
        @pl.when(jnp.logical_or(index // 2 != depth, lax.rem(index, 2) != core))
        def _():
            pl.semaphore_signal(
                barrier,
                inc=1,
                device_id={"freq": index // 2, "tile": chip * 2 + lax.rem(index, 2)},
                device_id_type=MESH,
            )

        return carry

    for copy in raws[:2] + small + raws[2:]:
        copy.start()
    lax.fori_loop(0, blocks, greet_tile, 0)
    lax.fori_loop(0, slots, greet_freq, 0)

    def reorder(slot, target):
        def widen(row, carry):
            for step in range(8):
                spread[pl.ds((row * 8 + step) * PITCH, blocks), :] = raw[
                    slot, row * 8 + step
                ].astype(jnp.float32)
            return carry

        lax.fori_loop(0, ROWS // 8, widen, 0)

        def narrow(index, carry):
            for step in range(2):
                target[index * 2 + step] = spread[
                    pl.ds(index * 2 + step, ROWS, stride=PITCH), :
                ].astype(jnp.bfloat16)
            return carry

        lax.fori_loop(0, blocks // 2, narrow, 0)

    raws[0].wait()
    raws[1].wait()
    reorder(other, right_out)
    reorder(core, right_all.at[core])
    small[0].wait()
    joined_out[...] = jnp.concatenate([direct[other, 0], direct[other, 1]], axis=0).astype(
        jnp.bfloat16
    )
    joined[core] = jnp.concatenate([direct[core, 0], direct[core, 1]], axis=0).astype(jnp.bfloat16)
    pl.semaphore_wait(barrier, blocks - 1 + slots - 1)

    lane = lax.broadcasted_iota(jnp.int32, (HALF, LANES), 1)
    column = lax.rem(lane, HALF)

    def products(fields, factors, side, first, signum):
        count = fields.shape[0] // 2
        low = lax.broadcasted_iota(jnp.int32, (count, LANES), 1) < HALF
        wide = jnp.concatenate([factors[side, first + step] for step in range(nx)], axis=1)
        result = jnp.dot(fields, wide, preferred_element_type=jnp.float32)
        pieces = []
        for step in range(nx):
            real = result[:count, step * LANES : (step + 1) * LANES]
            turned = roll_half(result[count:, step * LANES : (step + 1) * LANES])
            if signum > 0:
                piece = jnp.where(low, real - turned, turned + real)
            else:
                piece = jnp.where(low, real + turned, turned - real)
            pieces.append(piece.astype(jnp.bfloat16))
        return pieces

    def row_of(step, sign):
        reach = ny // 2 - (step + 1) // 2
        offset = jnp.where(lax.rem(step, 2) == 1, reach, ny - reach)
        return lax.rem(chip_y + ny + sign * offset, ny)

    def block_of(first, step):
        offsets = [*range(nx // 2, 0, -1), *range(nx // 2 + 1, nx), 0]
        return first + lax.rem(chip_x + offsets[step], nx)

    pair = remote(joined_out, joined.at[core], pair_send, pair_recv, partner)

    def factor_copy(step, source, target, send, recv):
        first = row_of(step, 1) * nx
        return remote(
            source.at[pl.ds(first, nx)],
            target.at[core, pl.ds(first, nx)],
            send,
            recv.at[step],
            partner,
        )

    def factor_wait(step, source, target, send, recv):
        first = row_of(step, 1) * nx
        remote(
            source.at[pl.ds(first, nx)],
            target.at[other, pl.ds(first, nx)],
            send,
            recv.at[step],
            partner,
        ).wait_recv()

    def start_right(step, carry):
        factor_copy(step, right_out, right_all, right_send, right_recv).start()
        return carry

    pair.start()
    lax.fori_loop(0, ny, start_right, 0)
    own_fields = joined[core]

    def own_group(index, carry):
        for step in range(2):
            first = (index * 2 + step) * nx
            pieces = products(own_fields, right_all, core, first, 1.0)
            for position in range(nx):
                partial[first + position] = pieces[position]
        return carry

    lax.fori_loop(0, ny // 2, own_group, 0)
    for copy in small[1:]:
        copy.wait()
    remote(joined_out, joined.at[other], pair_send, pair_recv, partner).wait_recv()

    def tile_copy(block, phase, part):
        where = pl.ds(part * PART, PART)
        return remote(
            sent.at[phase, block, where],
            got.at[phase, chip, where],
            tile_send.at[phase, part],
            tile_recv.at[phase, part, chip],
            {"freq": depth, "tile": block * 2 + core},
        )

    def send_group(first, phase, part):
        for step in range(nx):
            block = block_of(first, step)

            @pl.when(block != chip)
            def _():
                tile_copy(block, phase, part).start()

    other_fields = joined[other]

    def forward_group(index, carry):
        for inner in range(2):
            factor_wait(index * 2 + inner, right_out, right_all, right_send, right_recv)
        for inner in range(2):
            first = row_of(index * 2 + inner, 1) * nx
            pieces = products(other_fields, right_all, other, first, 1.0)
            for position in range(nx):
                block = first + position
                summed = pieces[position].astype(jnp.float32) + partial[block].astype(jnp.float32)
                value = jnp.where(column < ranks[core, block, chip], summed, 0.0)
                sent[0, block] = value.astype(jnp.bfloat16)
        for inner in range(2):
            send_group(row_of(index * 2 + inner, 1) * nx, 0, 0)
        return carry

    lax.fori_loop(0, ny // 2, forward_group, 0)
    got[0, chip] = sent[0, chip]
    for part in range(1, CHUNKS):

        def forward_rest(step, carry, part=part):
            send_group(row_of(step, 1) * nx, 0, part)
            return carry

        lax.fori_loop(0, ny, forward_rest, 0)
    raws[2].wait()
    raws[3].wait()
    reorder(2 + other, left_out)

    def start_left(step, carry):
        factor_copy(step, left_out, left_all, left_send, left_recv).start()
        return carry

    lax.fori_loop(0, ny, start_left, 0)
    reorder(2 + core, left_all.at[core])
    turn = 2 * samples_count
    place = lax.broadcasted_iota(jnp.int32, (steps, LANES), 1)
    moment = lax.broadcasted_iota(jnp.int32, (steps, LANES), 0) * CHUNKS + lax.rem(
        place // PART, CHUNKS
    )
    shift = jnp.where(place < HALF, 0, samples_count // 2)

    def weight(slot, carry):
        phase = lax.rem(moment * (2 * order[slot] + 1) + shift, turn)
        weights[slot] = jnp.cos(phase.astype(jnp.float32) * (2.0 * math.pi / turn))
        return carry

    lax.fori_loop(0, slots, weight, 0)
    late = lax.rem(lax.broadcasted_iota(jnp.int32, (rows_each, LANES), 1) // PART, CHUNKS)
    for part in range(CHUNKS):
        lane_window = window[:, part * PART : (part + 1) * PART]
        limits[part] = jnp.concatenate([lane_window] * (LANES // PART), axis=1) - late

    def wait_left(step, carry):
        factor_wait(step, left_out, left_all, left_send, left_recv)
        return carry

    lax.fori_loop(0, ny, wait_left, 0)

    def finish(phase, part, factors, signum):
        where = slice(part * PART, (part + 1) * PART)
        side_low = lax.broadcasted_iota(jnp.int32, (PART, LANES), 1) < HALF
        top_sign = jnp.where(side_low, 1.0, -signum)
        bottom_sign = jnp.where(side_low, 1.0, signum)

        def group(index, carry):
            members = []
            for inner in range(span):
                first = row_of(index * span + inner, -1) * nx
                members += [first + position for position in range(nx)]
            for block in members:

                @pl.when(block != chip)
                def _(block=block):
                    remote(
                        sent.at[phase, block, where],
                        got.at[phase, block, where],
                        tile_send.at[phase, part],
                        tile_recv.at[phase, part, block],
                        partner,
                    ).wait_recv()

            columns = []
            for block in members:
                piece = got[phase, block, where].astype(jnp.float32)
                top = (piece * top_sign).astype(jnp.bfloat16)
                bottom = (roll_half(piece) * bottom_sign).astype(jnp.bfloat16)
                columns.append(jnp.concatenate([top] * CHUNKS + [bottom] * CHUNKS, axis=0))
            wide = jnp.concatenate(columns, axis=1)
            for side in range(2):
                rows = jnp.concatenate([factors[side, block] for block in members], axis=1)
                value = lax.dot_general(
                    rows, wide, (((1,), (1,)), ((), ())), preferred_element_type=jnp.float32
                )
                total[side] = total[side] + value
            return carry

        span = max(1, ny // 2)
        total[...] = jnp.zeros_like(total)
        lax.fori_loop(0, ny // span, group, 0)

    def to_owner(index, phase, part):
        return remote(
            image.at[phase, part, index],
            gathered.at[phase, part, slot_here],
            freq_send.at[phase, part],
            freq_recv.at[phase, part],
            {"freq": lax.rem(index, nz), "tile": chip * 2 + index // nz},
        )

    def spread_image(phase, part):
        image[phase, part] = total[...].reshape(slots, rows_each, LANES).astype(jnp.bfloat16)

        def one(step, carry):
            level = lax.rem(step + depth + nz // 2, nz)
            for side in range(2):

                @pl.when(jnp.logical_or(level != depth, side != core))
                def _():
                    to_owner(side * nz + level, phase, part).start()

            return carry

        lax.fori_loop(0, nz, one, 0)
        gathered[phase, part, slot_here] = image[phase, part, mine]

    def many(source, target, send, recv, count):
        return remote(source.at[pl.ds(0, count)], target.at[pl.ds(0, count)], send, recv, partner)

    def freq_many(phase, part):
        return many(
            image.at[phase, part],
            gathered.at[phase, part],
            freq_send.at[phase, part],
            freq_recv.at[phase, part],
            slots - 1,
        )

    def mute(phase, part):
        limit = limits[part]
        values = [gathered[phase, part, slot].astype(jnp.float32) for slot in range(slots)]

        many_steps = min(8, steps)

        def invert(index, carry):
            for inner in range(many_steps):
                step = index * many_steps + inner
                sums = values[0] * weights[0, pl.ds(step, 1), :]
                for slot in range(1, slots):
                    sums = sums + values[slot] * weights[slot, pl.ds(step, 1), :]
                sums = (sums + roll_half(sums)) * (2.0 / samples_count)
                samples[step] = jnp.where(step * CHUNKS < limit, sums, 0.0)
            return carry

        lax.fori_loop(0, steps // many_steps, invert, 0)

        many_slots = min(8, slots)

        def forward(index, carry):
            for inner in range(many_slots):
                slot = index * many_slots + inner
                sums = samples[0] * weights[slot, pl.ds(0, 1), :]
                for step in range(1, steps):
                    sums = sums + samples[step] * weights[slot, pl.ds(step, 1), :]
                for group in range(1, CHUNKS):
                    sums = sums + pltpu.roll(sums, LANES - group * PART, 1)
                muted[phase, part, slot] = sums.astype(jnp.bfloat16)
            return carry

        lax.fori_loop(0, slots // many_slots, forward, 0)

    def to_slot(level, side, part):
        return remote(
            muted.at[0, part, level * 2 + side],
            focus.at[part, mine],
            back_send.at[0, part],
            back_recv.at[0, part],
            {"freq": level, "tile": chip * 2 + side},
        )

    def send_back(part):
        def one(step, carry):
            level = lax.rem(step + depth + nz // 2, nz)
            for side in range(2):

                @pl.when(jnp.logical_or(level != depth, side != core))
                def _():
                    to_slot(level, side, part).start()

            return carry

        lax.fori_loop(0, nz, one, 0)
        focus[part, mine] = muted[0, part, slot_here]

    def back_many(part):
        return many(
            muted.at[0, part],
            focus.at[part],
            back_send.at[0, part],
            back_recv.at[0, part],
            slots - 1,
        )

    def valid_rows(value):
        return jnp.concatenate([value[:PART], value[HALF : HALF + PART]], axis=0)

    def backward(part):
        fields = []
        for side in range(2):
            value = focus[part, side * nz : (side + 1) * nz].reshape(ROWS, LANES)
            fields.append(valid_rows(value.astype(jnp.float32).T).astype(jnp.bfloat16))
            swap_out[part, side] = fields[side]

        def one(index, carry):
            for inner in range(2):
                first = row_of(index * 2 + inner, 1) * nx
                lower = products(fields[0], left_all, 0, first, -1.0)
                upper = products(fields[1], left_all, 1, first, -1.0)
                for position in range(nx):
                    block = first + position
                    summed = lower[position].astype(jnp.float32)
                    summed = summed + upper[position].astype(jnp.float32)
                    kept = column[:PART] < ranks[core, chip, block]
                    value = jnp.where(kept, summed, 0.0).astype(jnp.bfloat16)
                    sent[1, block, slice(part * PART, (part + 1) * PART)] = value
            for inner in range(2):
                send_group(row_of(index * 2 + inner, 1) * nx, 1, part)
            return carry

        lax.fori_loop(0, ny // 2, one, 0)
        where = slice(part * PART, (part + 1) * PART)
        got[1, chip, where] = sent[1, chip, where]

    def swap(part):
        return remote(
            swap_out.at[part, other],
            swap_in.at[part],
            swap_send.at[part],
            swap_recv.at[part],
            partner,
        )

    def to_level(level, part):
        return remote(
            muted.at[1, part, pl.ds(level * 2, 2)],
            final.at[part, pl.ds(depth * 2, 2)],
            back_send.at[1, part],
            back_recv.at[1, part],
            {"freq": level, "tile": tile},
        )

    def send_final(part):
        def one(step, carry):
            level = lax.rem(step + depth + nz // 2, nz)

            @pl.when(level != depth)
            def _():
                to_level(level, part).start()

            return carry

        lax.fori_loop(0, nz, one, 0)
        final[part, pl.ds(depth * 2, 2)] = muted[1, part, pl.ds(depth * 2, 2)]

    def final_many(part):
        return many(
            muted.at[1, part],
            final.at[part],
            back_send.at[1, part],
            back_recv.at[1, part],
            slots - 2,
        )

    def tile_many(phase, part):
        where = pl.ds(part * PART, PART)
        return remote(
            sent.at[phase, pl.ds(0, blocks - 1), where],
            got.at[phase, pl.ds(0, blocks - 1), where],
            tile_send.at[phase, part],
            tile_recv.at[phase, part, 0],
            partner,
        )

    def store_plus(part):
        where = slice(part * PART, (part + 1) * PART)
        for slot in range(2):
            value = jnp.concatenate([final[part, 2 * level + slot] for level in range(nz)], axis=0)
            value = valid_rows(value.astype(jnp.float32).T).astype(plus_stage.dtype)
            plus_stage[slot, 0, where] = value[:PART]
            plus_stage[slot, 1, where] = value[PART:]

    for part in range(CHUNKS):
        finish(0, part, left_all, 1.0)
        spread_image(0, part)
        if part > 0:
            back_many(part - 1).wait_recv()
            backward(part - 1)
        freq_many(0, part).wait_recv()
        mute(0, part)
        send_back(part)
    back_many(CHUNKS - 1).wait_recv()
    backward(CHUNKS - 1)
    for part in range(CHUNKS):
        finish(1, part, right_all, -1.0)
        spread_image(1, part)
        if part > 0:
            final_many(part - 1).wait_recv()
            store_plus(part - 1)
            tile_many(1, part - 1).wait_send()
        if part == 0:
            for piece in range(CHUNKS):
                swap(piece).start()
            for piece in range(CHUNKS):
                rows = slice(piece * PART, (piece + 1) * PART)
                own = swap_out[piece, core]
                minus_stage[core, 0, rows] = own[:PART]
                minus_stage[core, 1, rows] = own[PART:]
                swap(piece).wait_recv()
                theirs = swap_in[piece]
                minus_stage[other, 0, rows] = theirs[:PART]
                minus_stage[other, 1, rows] = theirs[PART:]
            minus_copy = local(minus_stage, minus_hbm, out_sem.at[0])
            minus_copy.start()
            for piece in range(CHUNKS):
                tile_many(0, piece).wait_send()
                freq_many(0, piece).wait_send()
                back_many(piece).wait_send()
                swap(piece).wait_send()
            pair.wait_send()
            remote(right_out, right_all.at[core], right_send, right_recv.at[0], partner).wait_send()
            remote(left_out, left_all.at[core], left_send, left_recv.at[0], partner).wait_send()
        freq_many(1, part).wait_recv()
        mute(1, part)
        send_final(part)
    tile_many(1, CHUNKS - 1).wait_send()
    for part in range(CHUNKS):
        freq_many(1, part).wait_send()
    minus_copy.wait()
    final_many(CHUNKS - 1).wait_recv()
    store_plus(CHUNKS - 1)
    plus_copy = local(plus_stage, plus_hbm, out_sem.at[1])
    plus_copy.start()
    for part in range(CHUNKS):
        final_many(part).wait_send()
    plus_copy.wait()


def shards(dims, left_factor, right_factor, tile_ranks, freq_order, mute_window, direct_wave):
    ny, nx, nz, samples_count = dims
    blocks = ny * nx
    slots = 2 * nz
    rows_each = ROWS // nz
    bf16, f32 = jnp.bfloat16, jnp.float32
    dma = pltpu.SemaphoreType.DMA
    turned = jnp.transpose(direct_wave, (0, 1, 3, 2))
    factor = (2, blocks, ROWS, LANES)
    tiles = (blocks, FOCAL, LANES)
    pieces = (2, CHUNKS, slots, rows_each, LANES)
    stage = (2, 2, FOCAL, ROWS)
    each = (2, CHUNKS)
    scratch = [
        pltpu.VMEM((4, ROWS, blocks, LANES), bf16),
        pltpu.VMEM((ROWS * PITCH, LANES), f32),
        pltpu.VMEM(factor, bf16),
        pltpu.VMEM(factor, bf16),
        pltpu.VMEM(factor[1:], bf16),
        pltpu.VMEM(factor[1:], bf16),
        pltpu.VMEM(stage, f32),
        pltpu.VMEM(mute_window.shape, jnp.int32),
        pltpu.VMEM((CHUNKS, rows_each, LANES), jnp.int32),
        pltpu.SMEM(tile_ranks.shape, jnp.int32),
        pltpu.SMEM(freq_order.shape, jnp.int32),
        pltpu.VMEM((2, LANES, ROWS), bf16),
        pltpu.VMEM((LANES, ROWS), bf16),
        pltpu.VMEM(tiles, bf16),
        pltpu.VMEM((2,) + tiles, bf16),
        pltpu.VMEM((2,) + tiles, bf16),
        pltpu.VMEM((2, ROWS, LANES), f32),
        pltpu.VMEM(pieces, bf16),
        pltpu.VMEM(pieces, bf16),
        pltpu.VMEM((slots, samples_count // CHUNKS, LANES), f32),
        pltpu.VMEM((samples_count // CHUNKS, rows_each, LANES), f32),
        pltpu.VMEM(pieces, bf16),
        pltpu.VMEM(pieces[1:], bf16),
        pltpu.VMEM((CHUNKS, 2, 2 * PART, ROWS), bf16),
        pltpu.VMEM((CHUNKS, 2 * PART, ROWS), bf16),
        pltpu.VMEM(pieces[1:], bf16),
        pltpu.VMEM(stage, bf16),
        pltpu.VMEM(stage, bf16),
        dma((4,)),
        dma((4,)),
        dma((2,)),
        dma,
        dma,
        dma((CHUNKS,)),
        dma((CHUNKS,)),
        dma,
        dma((ny,)),
        dma,
        dma((ny,)),
        dma(each),
        dma(each + (blocks,)),
        dma(each),
        dma(each),
        dma(each),
        dma(each),
    ]
    out = jax.ShapeDtypeStruct(stage, bf16)
    plus, minus = pl.pallas_call(
        functools.partial(kernel, dims),
        out_shape=(out, out),
        in_specs=[pl.BlockSpec(memory_space=pltpu.HBM)] * 6,
        out_specs=(pl.BlockSpec(memory_space=pl.ANY),) * 2,
        scratch_shapes=scratch,
        compiler_params=pltpu.CompilerParams(
            collective_id=0, has_side_effects=True, vmem_limit_bytes=66000000
        ),
        name="focusing",
    )(right_factor, left_factor, tile_ranks, freq_order, mute_window, turned)
    plus = jnp.transpose(turned + plus.astype(f32), (0, 1, 3, 2))
    return plus, jnp.transpose(minus.astype(f32), (0, 1, 3, 2))


def solution(mesh):
    nz = mesh.shape["freq"]
    ny, nx = GRID[mesh.shape["tile"]]
    dims = (ny, nx, nz, 4 * nz)
    return jax.shard_map(
        functools.partial(shards, dims),
        mesh=mesh,
        in_specs=(
            P("freq", "tile", None, None),
            P("freq", "tile", None, None),
            P("freq", None, None),
            P(),
            P(("tile", "freq"), None),
            P("freq", None, "tile", None),
        ),
        out_specs=(P("freq", None, "tile", None), P("freq", None, "tile", None)),
        check_vma=False,
    )
```

```python
import functools
import math

import jax
import jax.numpy as jnp
from jax import lax
from jax.experimental import pallas as pl
from jax.experimental.pallas import tpu as pltpu
from jax.sharding import PartitionSpec as P

GRID = {64: (8, 4), 8: (2, 2)}
PITCH = 40
CHUNKS = 2
FOCAL = 64
PART = FOCAL // CHUNKS
CHUNKS = 2
FOCAL = 64
PART = FOCAL // CHUNKS
CHUNKS = 2
FOCAL = 64
PART = FOCAL // CHUNKS
CHUNKS = 2
FOCAL = 64
PART = FOCAL // CHUNKS
ROWS = 128
LANES = 128
HALF = 64
MESH = pl.DeviceIdType.MESH


def roll_half(value):
    return pltpu.roll(value, HALF, 1)


def kernel(
    dims,
    right_hbm,
    left_hbm,
    ranks_hbm,
    order_hbm,
    window_hbm,
    direct_hbm,
    both_hbm,
    raw,
    spread,
    right_all,
    left_all,
    right_out,
    left_out,
    direct,
    window,
    limits,
    ranks,
    order,
    joined,
    joined_out,
    partial,
    sent,
    got,
    total,
    image,
    gathered,
    weights,
    samples,
    muted,
    focus,
    swap_out,
    swap_in,
    final,
    minus_stage,
    plus_stage,
    raw_sem,
    in_sem,
    out_sem,
    pair_send,
    pair_recv,
    swap_send,
    swap_recv,
    right_send,
    right_recv,
    left_send,
    left_recv,
    tile_send,
    tile_recv,
    freq_send,
    freq_recv,
    back_send,
    back_recv,
):
    ny, nx, nz, samples_count = dims
    blocks = ny * nx
    slots = 2 * nz
    rows_each = ROWS // nz
    steps = samples_count // CHUNKS
    depth = lax.axis_index("freq")
    tile = lax.axis_index("tile")
    core = lax.rem(tile, 2)
    other = 1 - core
    chip = tile // 2
    chip_y = chip // nx
    chip_x = lax.rem(chip, nx)
    partner = {"freq": depth, "tile": tile + other - core}
    mine = core * nz + depth
    slot_here = 2 * depth + core

    def local(source, target, sem):
        return pltpu.make_async_copy(source, target, sem)

    def remote(source, target, send, recv, device):
        return pltpu.make_async_remote_copy(
            src_ref=source,
            dst_ref=target,
            send_sem=send,
            recv_sem=recv,
            device_id=device,
            device_id_type=MESH,
        )

    small = [
        local(direct_hbm, direct, in_sem.at[0]),
        local(window_hbm, window, in_sem.at[1]),
        local(ranks_hbm, ranks, in_sem.at[2]),
        local(order_hbm, order, in_sem.at[3]),
    ]
    raws = [
        local(right_hbm.at[0], raw.at[0], raw_sem.at[0]),
        local(right_hbm.at[1], raw.at[1], raw_sem.at[1]),
        local(left_hbm.at[0], raw.at[2], raw_sem.at[2]),
        local(left_hbm.at[1], raw.at[3], raw_sem.at[3]),
    ]
    barrier = pltpu.get_barrier_semaphore()

    def greet_tile(index, carry):
        @pl.when(index != chip)
        def _():
            pl.semaphore_signal(
                barrier,
                inc=1,
                device_id={"freq": depth, "tile": index * 2 + core},
                device_id_type=MESH,
            )

        return carry

    def greet_freq(index, carry):
        @pl.when(jnp.logical_or(index // 2 != depth, lax.rem(index, 2) != core))
        def _():
            pl.semaphore_signal(
                barrier,
                inc=1,
                device_id={"freq": index // 2, "tile": chip * 2 + lax.rem(index, 2)},
                device_id_type=MESH,
            )

        return carry

    for copy in raws[:2] + small + raws[2:]:
        copy.start()
    lax.fori_loop(0, blocks, greet_tile, 0)
    lax.fori_loop(0, slots, greet_freq, 0)

    def reorder(slot, target):
        def widen(row, carry):
            for step in range(8):
                spread[pl.ds((row * 8 + step) * PITCH, blocks), :] = raw[
                    slot, row * 8 + step
                ].astype(jnp.float32)
            return carry

        lax.fori_loop(0, ROWS // 8, widen, 0)

        def narrow(index, carry):
            for step in range(2):
                target[index * 2 + step] = spread[
                    pl.ds(index * 2 + step, ROWS, stride=PITCH), :
                ].astype(jnp.bfloat16)
            return carry

        lax.fori_loop(0, blocks // 2, narrow, 0)

    raws[0].wait()
    raws[1].wait()
    reorder(other, right_out)
    reorder(core, right_all.at[core])
    small[0].wait()
    joined_out[...] = jnp.concatenate([direct[other, 0], direct[other, 1]], axis=0).astype(
        jnp.bfloat16
    )
    joined[core] = jnp.concatenate([direct[core, 0], direct[core, 1]], axis=0).astype(jnp.bfloat16)
    pl.semaphore_wait(barrier, blocks - 1 + slots - 1)

    lane = lax.broadcasted_iota(jnp.int32, (HALF, LANES), 1)
    column = lax.rem(lane, HALF)

    def products(fields, factors, side, first, signum):
        count = fields.shape[0] // 2
        low = lax.broadcasted_iota(jnp.int32, (count, LANES), 1) < HALF
        wide = jnp.concatenate([factors[side, first + step] for step in range(nx)], axis=1)
        result = jnp.dot(fields, wide, preferred_element_type=jnp.float32)
        pieces = []
        for step in range(nx):
            real = result[:count, step * LANES : (step + 1) * LANES]
            turned = roll_half(result[count:, step * LANES : (step + 1) * LANES])
            if signum > 0:
                piece = jnp.where(low, real - turned, turned + real)
            else:
                piece = jnp.where(low, real + turned, turned - real)
            pieces.append(piece.astype(jnp.bfloat16))
        return pieces

    def row_of(step, sign):
        reach = ny // 2 - (step + 1) // 2
        offset = jnp.where(lax.rem(step, 2) == 1, reach, ny - reach)
        return lax.rem(chip_y + ny + sign * offset, ny)

    def level_of(step):
        reach = nz // 2 - (step + 1) // 2
        return lax.rem(depth + jnp.where(lax.rem(step, 2) == 1, reach, nz - reach), nz)

    def block_of(first, step):
        offsets = [*range(nx // 2, 0, -1), *range(nx // 2 + 1, nx), 0]
        return first + lax.rem(chip_x + offsets[step], nx)

    pair = remote(joined_out, joined.at[core], pair_send, pair_recv, partner)

    def factor_copy(step, source, target, send, recv):
        first = row_of(step, 1) * nx
        return remote(
            source.at[pl.ds(first, nx)],
            target.at[core, pl.ds(first, nx)],
            send,
            recv.at[step],
            partner,
        )

    def factor_wait(step, source, target, send, recv):
        first = row_of(step, 1) * nx
        remote(
            source.at[pl.ds(first, nx)],
            target.at[other, pl.ds(first, nx)],
            send,
            recv.at[step],
            partner,
        ).wait_recv()

    def start_right(step, carry):
        factor_copy(step, right_out, right_all, right_send, right_recv).start()
        return carry

    pair.start()
    lax.fori_loop(0, ny, start_right, 0)
    own_fields = joined[core]

    def own_group(index, carry):
        for step in range(2):
            first = (index * 2 + step) * nx
            pieces = products(own_fields, right_all, core, first, 1.0)
            for position in range(nx):
                partial[first + position] = pieces[position]
        return carry

    lax.fori_loop(0, ny // 2, own_group, 0)
    for copy in small[1:]:
        copy.wait()
    remote(joined_out, joined.at[other], pair_send, pair_recv, partner).wait_recv()

    def tile_copy(block, phase, part):
        where = pl.ds(part * PART, PART)
        return remote(
            sent.at[phase, block, where],
            got.at[phase, chip, where],
            tile_send.at[phase, part],
            tile_recv.at[phase, part, chip],
            {"freq": depth, "tile": block * 2 + core},
        )

    def send_group(first, phase, part):
        for step in range(nx):
            block = block_of(first, step)

            @pl.when(block != chip)
            def _():
                tile_copy(block, phase, part).start()

    other_fields = joined[other]

    def forward_group(index, carry):
        for inner in range(2):
            factor_wait(index * 2 + inner, right_out, right_all, right_send, right_recv)
        for inner in range(2):
            first = row_of(index * 2 + inner, 1) * nx
            pieces = products(other_fields, right_all, other, first, 1.0)
            for position in range(nx):
                block = first + position
                summed = pieces[position].astype(jnp.float32) + partial[block].astype(jnp.float32)
                value = jnp.where(column < ranks[core, block, chip], summed, 0.0)
                sent[0, block] = value.astype(jnp.bfloat16)
        for inner in range(2):
            send_group(row_of(index * 2 + inner, 1) * nx, 0, 0)
        return carry

    lax.fori_loop(0, ny // 2, forward_group, 0)
    got[0, chip] = sent[0, chip]
    for part in range(1, CHUNKS):

        def forward_rest(step, carry, part=part):
            send_group(row_of(step, 1) * nx, 0, part)
            return carry

        lax.fori_loop(0, ny, forward_rest, 0)
    raws[2].wait()
    raws[3].wait()
    reorder(2 + other, left_out)

    def start_left(step, carry):
        factor_copy(step, left_out, left_all, left_send, left_recv).start()
        return carry

    lax.fori_loop(0, ny, start_left, 0)
    reorder(2 + core, left_all.at[core])
    turn = 2 * samples_count
    place = lax.broadcasted_iota(jnp.int32, (steps, LANES), 1)
    moment = lax.broadcasted_iota(jnp.int32, (steps, LANES), 0) * CHUNKS + lax.rem(
        place // PART, CHUNKS
    )
    shift = jnp.where(place < HALF, 0, samples_count // 2)

    def weight(slot, carry):
        phase = lax.rem(moment * (2 * order[slot] + 1) + shift, turn)
        weights[slot] = jnp.cos(phase.astype(jnp.float32) * (2.0 * math.pi / turn))
        return carry

    lax.fori_loop(0, slots, weight, 0)
    late = lax.rem(lax.broadcasted_iota(jnp.int32, (rows_each, LANES), 1) // PART, CHUNKS)
    for part in range(CHUNKS):
        lane_window = window[:, part * PART : (part + 1) * PART]
        limits[part] = jnp.concatenate([lane_window] * (LANES // PART), axis=1) - late

    def wait_left(step, carry):
        factor_wait(step, left_out, left_all, left_send, left_recv)
        return carry

    lax.fori_loop(0, ny, wait_left, 0)

    def finish(phase, part, factors, signum):
        where = slice(part * PART, (part + 1) * PART)
        side_low = lax.broadcasted_iota(jnp.int32, (PART, LANES), 1) < HALF
        top_sign = jnp.where(side_low, 1.0, -signum)
        bottom_sign = jnp.where(side_low, 1.0, signum)

        def group(index, carry):
            members = []
            for inner in range(span):
                first = row_of(index * span + inner, -1) * nx
                members += [first + position for position in range(nx)]
            for block in members:

                @pl.when(block != chip)
                def _(block=block):
                    remote(
                        sent.at[phase, block, where],
                        got.at[phase, block, where],
                        tile_send.at[phase, part],
                        tile_recv.at[phase, part, block],
                        partner,
                    ).wait_recv()

            columns = []
            for block in members:
                piece = got[phase, block, where].astype(jnp.float32)
                top = (piece * top_sign).astype(jnp.bfloat16)
                bottom = (roll_half(piece) * bottom_sign).astype(jnp.bfloat16)
                columns.append(jnp.concatenate([top] * CHUNKS + [bottom] * CHUNKS, axis=0))
            wide = jnp.concatenate(columns, axis=1)
            for side in range(2):
                rows = jnp.concatenate([factors[side, block] for block in members], axis=1)
                value = lax.dot_general(
                    rows, wide, (((1,), (1,)), ((), ())), preferred_element_type=jnp.float32
                )
                total[side] = total[side] + value
            return carry

        span = max(1, ny // 2)
        total[...] = jnp.zeros_like(total)
        lax.fori_loop(0, ny // span, group, 0)

    def to_owner(index, phase, part):
        return remote(
            image.at[phase, part, index],
            gathered.at[phase, part, slot_here],
            freq_send.at[phase, part],
            freq_recv.at[phase, part],
            {"freq": lax.rem(index, nz), "tile": chip * 2 + index // nz},
        )

    def spread_image(phase, part):
        image[phase, part] = total[...].reshape(slots, rows_each, LANES).astype(jnp.bfloat16)

        def one(step, carry):
            level = level_of(step)
            for side in range(2):

                @pl.when(jnp.logical_or(level != depth, side != core))
                def _():
                    to_owner(side * nz + level, phase, part).start()

            return carry

        lax.fori_loop(0, nz, one, 0)
        gathered[phase, part, slot_here] = image[phase, part, mine]

    def many(source, target, send, recv, count):
        return remote(source.at[pl.ds(0, count)], target.at[pl.ds(0, count)], send, recv, partner)

    def freq_many(phase, part):
        return many(
            image.at[phase, part],
            gathered.at[phase, part],
            freq_send.at[phase, part],
            freq_recv.at[phase, part],
            slots - 1,
        )

    def mute(phase, part):
        limit = limits[part]
        values = [gathered[phase, part, slot].astype(jnp.float32) for slot in range(slots)]

        many_steps = min(8, steps)

        def invert(index, carry):
            for inner in range(many_steps):
                step = index * many_steps + inner
                sums = values[0] * weights[0, pl.ds(step, 1), :]
                for slot in range(1, slots):
                    sums = sums + values[slot] * weights[slot, pl.ds(step, 1), :]
                sums = (sums + roll_half(sums)) * (2.0 / samples_count)
                samples[step] = jnp.where(step * CHUNKS < limit, sums, 0.0)
            return carry

        lax.fori_loop(0, steps // many_steps, invert, 0)

        many_slots = min(8, slots)

        def forward(index, carry):
            for inner in range(many_slots):
                slot = index * many_slots + inner
                sums = samples[0] * weights[slot, pl.ds(0, 1), :]
                for step in range(1, steps):
                    sums = sums + samples[step] * weights[slot, pl.ds(step, 1), :]
                for group in range(1, CHUNKS):
                    sums = sums + pltpu.roll(sums, LANES - group * PART, 1)
                muted[phase, part, slot] = sums.astype(jnp.bfloat16)
            return carry

        lax.fori_loop(0, slots // many_slots, forward, 0)

    def to_slot(level, side, part):
        return remote(
            muted.at[0, part, level * 2 + side],
            focus.at[part, mine],
            back_send.at[0, part],
            back_recv.at[0, part],
            {"freq": level, "tile": chip * 2 + side},
        )

    def send_back(part):
        def one(step, carry):
            level = level_of(step)
            for side in range(2):

                @pl.when(jnp.logical_or(level != depth, side != core))
                def _():
                    to_slot(level, side, part).start()

            return carry

        lax.fori_loop(0, nz, one, 0)
        focus[part, mine] = muted[0, part, slot_here]

    def back_many(part):
        return many(
            muted.at[0, part],
            focus.at[part],
            back_send.at[0, part],
            back_recv.at[0, part],
            slots - 1,
        )

    def valid_rows(value):
        return jnp.concatenate([value[:PART], value[HALF : HALF + PART]], axis=0)

    def backward(part):
        fields = []
        for side in range(2):
            value = focus[part, side * nz : (side + 1) * nz].reshape(ROWS, LANES)
            fields.append(valid_rows(value.astype(jnp.float32).T).astype(jnp.bfloat16))
            swap_out[part, side] = fields[side]

        def one(index, carry):
            for inner in range(2):
                first = row_of(index * 2 + inner, 1) * nx
                lower = products(fields[0], left_all, 0, first, -1.0)
                upper = products(fields[1], left_all, 1, first, -1.0)
                for position in range(nx):
                    block = first + position
                    summed = lower[position].astype(jnp.float32)
                    summed = summed + upper[position].astype(jnp.float32)
                    kept = column[:PART] < ranks[core, chip, block]
                    value = jnp.where(kept, summed, 0.0).astype(jnp.bfloat16)
                    sent[1, block, slice(part * PART, (part + 1) * PART)] = value
            for inner in range(2):
                send_group(row_of(index * 2 + inner, 1) * nx, 1, part)
            return carry

        lax.fori_loop(0, ny // 2, one, 0)
        where = slice(part * PART, (part + 1) * PART)
        got[1, chip, where] = sent[1, chip, where]

    def swap(part):
        return remote(
            swap_out.at[part, other],
            swap_in.at[part],
            swap_send.at[part],
            swap_recv.at[part],
            partner,
        )

    def to_level(level, part):
        return remote(
            muted.at[1, part, pl.ds(level * 2, 2)],
            final.at[part, pl.ds(depth * 2, 2)],
            back_send.at[1, part],
            back_recv.at[1, part],
            {"freq": level, "tile": tile},
        )

    def send_final(part):
        def one(step, carry):
            level = level_of(step)

            @pl.when(level != depth)
            def _():
                to_level(level, part).start()

            return carry

        lax.fori_loop(0, nz, one, 0)
        final[part, pl.ds(depth * 2, 2)] = muted[1, part, pl.ds(depth * 2, 2)]

    def final_many(part):
        return many(
            muted.at[1, part],
            final.at[part],
            back_send.at[1, part],
            back_recv.at[1, part],
            slots - 2,
        )

    def tile_many(phase, part):
        where = pl.ds(part * PART, PART)
        return remote(
            sent.at[phase, pl.ds(0, blocks - 1), where],
            got.at[phase, pl.ds(0, blocks - 1), where],
            tile_send.at[phase, part],
            tile_recv.at[phase, part, 0],
            partner,
        )

    def store_plus(part):
        where = slice(part * PART, (part + 1) * PART)
        for slot in range(2):
            value = jnp.concatenate([final[part, 2 * level + slot] for level in range(nz)], axis=0)
            value = valid_rows(value.astype(jnp.float32).T).astype(plus_stage.dtype)
            plus_stage[slot, 0, where] = value[:PART]
            plus_stage[slot, 1, where] = value[PART:]

    for part in range(CHUNKS):
        finish(0, part, left_all, 1.0)
        spread_image(0, part)
        if part > 0:
            back_many(part - 1).wait_recv()
            backward(part - 1)
        freq_many(0, part).wait_recv()
        mute(0, part)
        send_back(part)
    back_many(CHUNKS - 1).wait_recv()
    backward(CHUNKS - 1)
    for part in range(CHUNKS):
        finish(1, part, right_all, -1.0)
        spread_image(1, part)
        if part > 0:
            final_many(part - 1).wait_recv()
            store_plus(part - 1)
            tile_many(1, part - 1).wait_send()
        if part == 0:
            for piece in range(CHUNKS):
                swap(piece).start()
            for piece in range(CHUNKS):
                rows = slice(piece * PART, (piece + 1) * PART)
                own = swap_out[piece, core]
                minus_stage[core, 0, rows] = own[:PART]
                minus_stage[core, 1, rows] = own[PART:]
                swap(piece).wait_recv()
                theirs = swap_in[piece]
                minus_stage[other, 0, rows] = theirs[:PART]
                minus_stage[other, 1, rows] = theirs[PART:]
            minus_copy = local(minus_stage, both_hbm.at[1], out_sem.at[0])
            minus_copy.start()
            for piece in range(CHUNKS):
                tile_many(0, piece).wait_send()
                freq_many(0, piece).wait_send()
                back_many(piece).wait_send()
                swap(piece).wait_send()
            pair.wait_send()
            remote(right_out, right_all.at[core], right_send, right_recv.at[0], partner).wait_send()
            remote(left_out, left_all.at[core], left_send, left_recv.at[0], partner).wait_send()
        freq_many(1, part).wait_recv()
        mute(1, part)
        send_final(part)
    tile_many(1, CHUNKS - 1).wait_send()
    for part in range(CHUNKS):
        freq_many(1, part).wait_send()
    minus_copy.wait()
    final_many(CHUNKS - 1).wait_recv()
    store_plus(CHUNKS - 1)
    plus_copy = local(plus_stage, both_hbm.at[0], out_sem.at[1])
    plus_copy.start()
    for part in range(CHUNKS):
        final_many(part).wait_send()
    plus_copy.wait()


def widen_results(both_hbm, direct_hbm, plus_hbm, minus_hbm, both, direct, wide, in_sem, out_sem):
    ins = [
        pltpu.make_async_copy(both_hbm.at[1], both.at[1], in_sem.at[0]),
        pltpu.make_async_copy(both_hbm.at[0], both.at[0], in_sem.at[1]),
        pltpu.make_async_copy(direct_hbm, direct, in_sem.at[2]),
    ]
    outs = [
        pltpu.make_async_copy(wide.at[1], minus_hbm, out_sem.at[0]),
        pltpu.make_async_copy(wide.at[0], plus_hbm, out_sem.at[1]),
    ]
    for copy in ins:
        copy.start()
    ins[0].wait()
    wide[1] = both[1].astype(jnp.float32)
    outs[0].start()
    ins[1].wait()
    ins[2].wait()
    wide[0] = direct[...] + both[0].astype(jnp.float32)
    outs[1].start()
    for copy in outs:
        copy.wait()


def shards(dims, left_factor, right_factor, tile_ranks, freq_order, mute_window, direct_wave):
    ny, nx, nz, samples_count = dims
    blocks = ny * nx
    slots = 2 * nz
    rows_each = ROWS // nz
    bf16, f32 = jnp.bfloat16, jnp.float32
    dma = pltpu.SemaphoreType.DMA
    turned = jnp.transpose(direct_wave, (0, 1, 3, 2))
    factor = (2, blocks, ROWS, LANES)
    tiles = (blocks, FOCAL, LANES)
    pieces = (2, CHUNKS, slots, rows_each, LANES)
    stage = (2, 2, FOCAL, ROWS)
    each = (2, CHUNKS)
    scratch = [
        pltpu.VMEM((4, ROWS, blocks, LANES), bf16),
        pltpu.VMEM((ROWS * PITCH, LANES), f32),
        pltpu.VMEM(factor, bf16),
        pltpu.VMEM(factor, bf16),
        pltpu.VMEM(factor[1:], bf16),
        pltpu.VMEM(factor[1:], bf16),
        pltpu.VMEM(stage, f32),
        pltpu.VMEM(mute_window.shape, jnp.int32),
        pltpu.VMEM((CHUNKS, rows_each, LANES), jnp.int32),
        pltpu.SMEM(tile_ranks.shape, jnp.int32),
        pltpu.SMEM(freq_order.shape, jnp.int32),
        pltpu.VMEM((2, LANES, ROWS), bf16),
        pltpu.VMEM((LANES, ROWS), bf16),
        pltpu.VMEM(tiles, bf16),
        pltpu.VMEM((2,) + tiles, bf16),
        pltpu.VMEM((2,) + tiles, bf16),
        pltpu.VMEM((2, ROWS, LANES), f32),
        pltpu.VMEM(pieces, bf16),
        pltpu.VMEM(pieces, bf16),
        pltpu.VMEM((slots, samples_count // CHUNKS, LANES), f32),
        pltpu.VMEM((samples_count // CHUNKS, rows_each, LANES), f32),
        pltpu.VMEM(pieces, bf16),
        pltpu.VMEM(pieces[1:], bf16),
        pltpu.VMEM((CHUNKS, 2, 2 * PART, ROWS), bf16),
        pltpu.VMEM((CHUNKS, 2 * PART, ROWS), bf16),
        pltpu.VMEM(pieces[1:], bf16),
        pltpu.VMEM(stage, bf16),
        pltpu.VMEM(stage, bf16),
        dma((4,)),
        dma((4,)),
        dma((2,)),
        dma,
        dma,
        dma((CHUNKS,)),
        dma((CHUNKS,)),
        dma,
        dma((ny,)),
        dma,
        dma((ny,)),
        dma(each),
        dma(each + (blocks,)),
        dma(each),
        dma(each),
        dma(each),
        dma(each),
    ]
    out = jax.ShapeDtypeStruct((2,) + stage, bf16)
    both = pl.pallas_call(
        functools.partial(kernel, dims),
        out_shape=out,
        in_specs=[pl.BlockSpec(memory_space=pltpu.HBM)] * 6,
        out_specs=pl.BlockSpec(memory_space=pl.ANY),
        scratch_shapes=scratch,
        compiler_params=pltpu.CompilerParams(
            collective_id=0, has_side_effects=True, vmem_limit_bytes=66000000
        ),
        name="focusing",
    )(right_factor, left_factor, tile_ranks, freq_order, mute_window, turned)
    wide = jax.ShapeDtypeStruct(stage, f32)
    plus, minus = pl.pallas_call(
        widen_results,
        out_shape=(wide, wide),
        in_specs=[pl.BlockSpec(memory_space=pl.ANY)] * 2,
        out_specs=(pl.BlockSpec(memory_space=pl.ANY),) * 2,
        scratch_shapes=[
            pltpu.VMEM((2,) + stage, bf16),
            pltpu.VMEM(stage, f32),
            pltpu.VMEM((2,) + stage, f32),
            dma((3,)),
            dma((2,)),
        ],
        compiler_params=pltpu.CompilerParams(vmem_limit_bytes=66000000),
        name="widen",
    )(both, turned)
    return jnp.transpose(plus, (0, 1, 3, 2)), jnp.transpose(minus, (0, 1, 3, 2))


def solution(mesh):
    nz = mesh.shape["freq"]
    ny, nx = GRID[mesh.shape["tile"]]
    dims = (ny, nx, nz, 4 * nz)
    return jax.shard_map(
        functools.partial(shards, dims),
        mesh=mesh,
        in_specs=(
            P("freq", "tile", None, None),
            P("freq", "tile", None, None),
            P("freq", None, None),
            P(),
            P(("tile", "freq"), None),
            P("freq", None, "tile", None),
        ),
        out_specs=(P("freq", None, "tile", None), P("freq", None, "tile", None)),
        check_vma=False,
    )
```

```python
import functools
import math

import jax
import jax.numpy as jnp
from jax import lax
from jax.experimental import pallas as pl
from jax.experimental.pallas import tpu as pltpu
from jax.sharding import PartitionSpec as P

GRID = {64: (8, 4), 8: (2, 2)}
PITCH = 40
CHUNKS = 2
FOCAL = 64
PART = FOCAL // CHUNKS
CHUNKS = 2
FOCAL = 64
PART = FOCAL // CHUNKS
CHUNKS = 2
FOCAL = 64
PART = FOCAL // CHUNKS
CHUNKS = 2
FOCAL = 64
PART = FOCAL // CHUNKS
ROWS = 128
LANES = 128
HALF = 64
MESH = pl.DeviceIdType.MESH


def roll_half(value):
    return pltpu.roll(value, HALF, 1)


def kernel(
    dims,
    right_hbm,
    left_hbm,
    ranks_hbm,
    order_hbm,
    window_hbm,
    direct_hbm,
    both_hbm,
    raw,
    spread,
    right_all,
    left_all,
    right_out,
    left_out,
    direct,
    window,
    limits,
    ranks,
    order,
    joined,
    joined_out,
    partial,
    sent,
    got,
    total,
    image,
    gathered,
    weights,
    samples,
    muted,
    focus,
    swap_out,
    swap_in,
    final,
    minus_stage,
    plus_stage,
    raw_sem,
    in_sem,
    out_sem,
    pair_send,
    pair_recv,
    swap_send,
    swap_recv,
    right_send,
    right_recv,
    left_send,
    left_recv,
    tile_send,
    tile_recv,
    freq_send,
    freq_recv,
    back_send,
    back_recv,
):
    ny, nx, nz, samples_count = dims
    blocks = ny * nx
    slots = 2 * nz
    rows_each = ROWS // nz
    steps = samples_count // CHUNKS
    depth = lax.axis_index("freq")
    tile = lax.axis_index("tile")
    core = lax.rem(tile, 2)
    other = 1 - core
    chip = tile // 2
    chip_y = chip // nx
    chip_x = lax.rem(chip, nx)
    partner = {"freq": depth, "tile": tile + other - core}
    mine = core * nz + depth
    slot_here = 2 * depth + core

    def local(source, target, sem):
        return pltpu.make_async_copy(source, target, sem)

    def remote(source, target, send, recv, device):
        return pltpu.make_async_remote_copy(
            src_ref=source,
            dst_ref=target,
            send_sem=send,
            recv_sem=recv,
            device_id=device,
            device_id_type=MESH,
        )

    small = [
        local(direct_hbm, direct, in_sem.at[0]),
        local(window_hbm, window, in_sem.at[1]),
        local(ranks_hbm, ranks, in_sem.at[2]),
        local(order_hbm, order, in_sem.at[3]),
    ]
    raws = [
        local(right_hbm.at[0], raw.at[0], raw_sem.at[0]),
        local(right_hbm.at[1], raw.at[1], raw_sem.at[1]),
        local(left_hbm.at[0], raw.at[2], raw_sem.at[2]),
        local(left_hbm.at[1], raw.at[3], raw_sem.at[3]),
    ]
    barrier = pltpu.get_barrier_semaphore()

    def row_of(step, sign):
        reach = ny // 2 - (step + 1) // 2
        offset = jnp.where(lax.rem(step, 2) == 1, reach, ny - reach)
        return lax.rem(chip_y + ny + sign * offset, ny)

    def level_of(step):
        reach = nz // 2 - (step + 1) // 2
        return lax.rem(depth + jnp.where(lax.rem(step, 2) == 1, reach, nz - reach), nz)

    def block_of(first, step):
        offsets = [*range(nx // 2, 0, -1), *range(nx // 2 + 1, nx), 0]
        return first + lax.rem(chip_x + offsets[step], nx)

    def greet_tile(step, carry):
        for inner in range(nx):
            block = block_of(row_of(step, 1) * nx, inner)

            @pl.when(block != chip)
            def _(block=block):
                pl.semaphore_signal(
                    barrier,
                    inc=1,
                    device_id={"freq": depth, "tile": block * 2 + core},
                    device_id_type=MESH,
                )

        return carry

    def greet_freq(step, carry):
        level = level_of(step)
        for side in range(2):

            @pl.when(jnp.logical_or(level != depth, side != core))
            def _(side=side):
                pl.semaphore_signal(
                    barrier,
                    inc=1,
                    device_id={"freq": level, "tile": chip * 2 + side},
                    device_id_type=MESH,
                )

        return carry

    for copy in raws[:2] + small + raws[2:]:
        copy.start()
    lax.fori_loop(0, ny, greet_tile, 0)
    lax.fori_loop(0, nz, greet_freq, 0)

    def reorder(slot, target):
        def widen(row, carry):
            for step in range(8):
                spread[pl.ds((row * 8 + step) * PITCH, blocks), :] = raw[
                    slot, row * 8 + step
                ].astype(jnp.float32)
            return carry

        lax.fori_loop(0, ROWS // 8, widen, 0)

        def narrow(index, carry):
            for step in range(2):
                target[index * 2 + step] = spread[
                    pl.ds(index * 2 + step, ROWS, stride=PITCH), :
                ].astype(jnp.bfloat16)
            return carry

        lax.fori_loop(0, blocks // 2, narrow, 0)

    raws[0].wait()
    raws[1].wait()
    reorder(other, right_out)
    reorder(core, right_all.at[core])
    small[0].wait()
    joined_out[...] = jnp.concatenate([direct[other, 0], direct[other, 1]], axis=0).astype(
        jnp.bfloat16
    )
    joined[core] = jnp.concatenate([direct[core, 0], direct[core, 1]], axis=0).astype(jnp.bfloat16)
    pl.semaphore_wait(barrier, blocks - 1 + slots - 1)

    lane = lax.broadcasted_iota(jnp.int32, (HALF, LANES), 1)
    column = lax.rem(lane, HALF)

    def products(fields, factors, side, first, signum):
        count = fields.shape[0] // 2
        low = lax.broadcasted_iota(jnp.int32, (count, LANES), 1) < HALF
        wide = jnp.concatenate([factors[side, first + step] for step in range(nx)], axis=1)
        result = jnp.dot(fields, wide, preferred_element_type=jnp.float32)
        pieces = []
        for step in range(nx):
            real = result[:count, step * LANES : (step + 1) * LANES]
            turned = roll_half(result[count:, step * LANES : (step + 1) * LANES])
            if signum > 0:
                piece = jnp.where(low, real - turned, turned + real)
            else:
                piece = jnp.where(low, real + turned, turned - real)
            pieces.append(piece.astype(jnp.bfloat16))
        return pieces

    pair = remote(joined_out, joined.at[core], pair_send, pair_recv, partner)

    def factor_copy(step, source, target, send, recv):
        first = row_of(step, 1) * nx
        return remote(
            source.at[pl.ds(first, nx)],
            target.at[core, pl.ds(first, nx)],
            send,
            recv.at[step],
            partner,
        )

    def factor_wait(step, source, target, send, recv):
        first = row_of(step, 1) * nx
        remote(
            source.at[pl.ds(first, nx)],
            target.at[other, pl.ds(first, nx)],
            send,
            recv.at[step],
            partner,
        ).wait_recv()

    def start_right(step, carry):
        factor_copy(step, right_out, right_all, right_send, right_recv).start()
        return carry

    pair.start()
    lax.fori_loop(0, ny, start_right, 0)
    own_fields = joined[core]

    def own_group(index, carry):
        for step in range(2):
            first = (index * 2 + step) * nx
            pieces = products(own_fields, right_all, core, first, 1.0)
            for position in range(nx):
                partial[first + position] = pieces[position]
        return carry

    lax.fori_loop(0, ny // 2, own_group, 0)
    for copy in small[1:]:
        copy.wait()
    remote(joined_out, joined.at[other], pair_send, pair_recv, partner).wait_recv()

    def tile_copy(block, phase, part):
        where = pl.ds(part * PART, PART)
        return remote(
            sent.at[phase, block, where],
            got.at[phase, chip, where],
            tile_send.at[phase, part],
            tile_recv.at[phase, part, chip],
            {"freq": depth, "tile": block * 2 + core},
        )

    def send_group(first, phase, part):
        for step in range(nx):
            block = block_of(first, step)

            @pl.when(block != chip)
            def _():
                tile_copy(block, phase, part).start()

    other_fields = joined[other]

    def forward_group(index, carry):
        for inner in range(2):
            factor_wait(index * 2 + inner, right_out, right_all, right_send, right_recv)
        for inner in range(2):
            first = row_of(index * 2 + inner, 1) * nx
            pieces = products(other_fields, right_all, other, first, 1.0)
            for position in range(nx):
                block = first + position
                summed = pieces[position].astype(jnp.float32) + partial[block].astype(jnp.float32)
                value = jnp.where(column < ranks[core, block, chip], summed, 0.0)
                sent[0, block] = value.astype(jnp.bfloat16)
        for inner in range(2):
            send_group(row_of(index * 2 + inner, 1) * nx, 0, 0)
        return carry

    lax.fori_loop(0, ny // 2, forward_group, 0)
    got[0, chip] = sent[0, chip]
    for part in range(1, CHUNKS):

        def forward_rest(step, carry, part=part):
            send_group(row_of(step, 1) * nx, 0, part)
            return carry

        lax.fori_loop(0, ny, forward_rest, 0)
    raws[2].wait()
    raws[3].wait()
    reorder(2 + other, left_out)

    def start_left(step, carry):
        factor_copy(step, left_out, left_all, left_send, left_recv).start()
        return carry

    lax.fori_loop(0, ny, start_left, 0)
    reorder(2 + core, left_all.at[core])
    turn = 2 * samples_count
    place = lax.broadcasted_iota(jnp.int32, (steps, LANES), 1)
    moment = lax.broadcasted_iota(jnp.int32, (steps, LANES), 0) * CHUNKS + lax.rem(
        place // PART, CHUNKS
    )
    shift = jnp.where(place < HALF, 0, samples_count // 2)

    def weight(slot, carry):
        phase = lax.rem(moment * (2 * order[slot] + 1) + shift, turn)
        weights[slot] = jnp.cos(phase.astype(jnp.float32) * (2.0 * math.pi / turn))
        return carry

    lax.fori_loop(0, slots, weight, 0)
    late = lax.rem(lax.broadcasted_iota(jnp.int32, (rows_each, LANES), 1) // PART, CHUNKS)
    for part in range(CHUNKS):
        lane_window = window[:, part * PART : (part + 1) * PART]
        limits[part] = jnp.concatenate([lane_window] * (LANES // PART), axis=1) - late

    def wait_left(step, carry):
        factor_wait(step, left_out, left_all, left_send, left_recv)
        return carry

    lax.fori_loop(0, ny, wait_left, 0)

    def finish(phase, part, factors, signum):
        where = slice(part * PART, (part + 1) * PART)
        side_low = lax.broadcasted_iota(jnp.int32, (PART, LANES), 1) < HALF
        top_sign = jnp.where(side_low, 1.0, -signum)
        bottom_sign = jnp.where(side_low, 1.0, signum)

        def group(index, carry):
            members = []
            for inner in range(span):
                first = row_of(index * span + inner, -1) * nx
                members += [first + position for position in range(nx)]
            for block in members:

                @pl.when(block != chip)
                def _(block=block):
                    remote(
                        sent.at[phase, block, where],
                        got.at[phase, block, where],
                        tile_send.at[phase, part],
                        tile_recv.at[phase, part, block],
                        partner,
                    ).wait_recv()

            columns = []
            for block in members:
                piece = got[phase, block, where].astype(jnp.float32)
                top = (piece * top_sign).astype(jnp.bfloat16)
                bottom = (roll_half(piece) * bottom_sign).astype(jnp.bfloat16)
                columns.append(jnp.concatenate([top] * CHUNKS + [bottom] * CHUNKS, axis=0))
            wide = jnp.concatenate(columns, axis=1)
            for side in range(2):
                rows = jnp.concatenate([factors[side, block] for block in members], axis=1)
                value = lax.dot_general(
                    rows, wide, (((1,), (1,)), ((), ())), preferred_element_type=jnp.float32
                )
                total[side] = total[side] + value
            return carry

        span = ny if part == CHUNKS - 1 else max(1, ny // 2)
        total[...] = jnp.zeros_like(total)
        lax.fori_loop(0, ny // span, group, 0)

    def to_owner(index, phase, part):
        return remote(
            image.at[phase, part, index],
            gathered.at[phase, part, slot_here],
            freq_send.at[phase, part],
            freq_recv.at[phase, part],
            {"freq": lax.rem(index, nz), "tile": chip * 2 + index // nz},
        )

    def spread_image(phase, part):
        image[phase, part] = total[...].reshape(slots, rows_each, LANES).astype(jnp.bfloat16)

        def one(step, carry):
            level = level_of(step)
            for side in range(2):

                @pl.when(jnp.logical_or(level != depth, side != core))
                def _():
                    to_owner(side * nz + level, phase, part).start()

            return carry

        lax.fori_loop(0, nz, one, 0)
        gathered[phase, part, slot_here] = image[phase, part, mine]

    def many(source, target, send, recv, count):
        return remote(source.at[pl.ds(0, count)], target.at[pl.ds(0, count)], send, recv, partner)

    def freq_many(phase, part):
        return many(
            image.at[phase, part],
            gathered.at[phase, part],
            freq_send.at[phase, part],
            freq_recv.at[phase, part],
            slots - 1,
        )

    def mute(phase, part):
        limit = limits[part]
        values = [gathered[phase, part, slot].astype(jnp.float32) for slot in range(slots)]

        many_steps = min(16, steps)

        def invert(index, carry):
            for inner in range(many_steps):
                step = index * many_steps + inner
                sums = values[0] * weights[0, pl.ds(step, 1), :]
                for slot in range(1, slots):
                    sums = sums + values[slot] * weights[slot, pl.ds(step, 1), :]
                sums = (sums + roll_half(sums)) * (2.0 / samples_count)
                samples[step] = jnp.where(step * CHUNKS < limit, sums, 0.0)
            return carry

        lax.fori_loop(0, steps // many_steps, invert, 0)

        many_slots = min(8, slots)

        def forward(index, carry):
            for inner in range(many_slots):
                slot = index * many_slots + inner
                sums = samples[0] * weights[slot, pl.ds(0, 1), :]
                for step in range(1, steps):
                    sums = sums + samples[step] * weights[slot, pl.ds(step, 1), :]
                for group in range(1, CHUNKS):
                    sums = sums + pltpu.roll(sums, LANES - group * PART, 1)
                muted[phase, part, slot] = sums.astype(jnp.bfloat16)
            return carry

        lax.fori_loop(0, slots // many_slots, forward, 0)

    def to_slot(level, side, part):
        return remote(
            muted.at[0, part, level * 2 + side],
            focus.at[part, mine],
            back_send.at[0, part],
            back_recv.at[0, part],
            {"freq": level, "tile": chip * 2 + side},
        )

    def send_back(part):
        def one(step, carry):
            level = level_of(step)
            for side in range(2):

                @pl.when(jnp.logical_or(level != depth, side != core))
                def _():
                    to_slot(level, side, part).start()

            return carry

        lax.fori_loop(0, nz, one, 0)
        focus[part, mine] = muted[0, part, slot_here]

    def back_many(part):
        return many(
            muted.at[0, part],
            focus.at[part],
            back_send.at[0, part],
            back_recv.at[0, part],
            slots - 1,
        )

    def valid_rows(value):
        return jnp.concatenate([value[:PART], value[HALF : HALF + PART]], axis=0)

    def backward(part):
        fields = []
        for side in range(2):
            value = focus[part, side * nz : (side + 1) * nz].reshape(ROWS, LANES)
            fields.append(valid_rows(value.astype(jnp.float32).T).astype(jnp.bfloat16))
            swap_out[part, side] = fields[side]

        def one(index, carry):
            for inner in range(2):
                first = row_of(index * 2 + inner, 1) * nx
                lower = products(fields[0], left_all, 0, first, -1.0)
                upper = products(fields[1], left_all, 1, first, -1.0)
                for position in range(nx):
                    block = first + position
                    summed = lower[position].astype(jnp.float32)
                    summed = summed + upper[position].astype(jnp.float32)
                    kept = column[:PART] < ranks[core, chip, block]
                    value = jnp.where(kept, summed, 0.0).astype(jnp.bfloat16)
                    sent[1, block, slice(part * PART, (part + 1) * PART)] = value
            for inner in range(2):
                send_group(row_of(index * 2 + inner, 1) * nx, 1, part)
            return carry

        lax.fori_loop(0, ny // 2, one, 0)
        where = slice(part * PART, (part + 1) * PART)
        got[1, chip, where] = sent[1, chip, where]

    def swap(part):
        return remote(
            swap_out.at[part, other],
            swap_in.at[part],
            swap_send.at[part],
            swap_recv.at[part],
            partner,
        )

    def to_level(level, part):
        return remote(
            muted.at[1, part, pl.ds(level * 2, 2)],
            final.at[part, pl.ds(depth * 2, 2)],
            back_send.at[1, part],
            back_recv.at[1, part],
            {"freq": level, "tile": tile},
        )

    def send_final(part):
        def one(step, carry):
            level = level_of(step)

            @pl.when(level != depth)
            def _():
                to_level(level, part).start()

            return carry

        lax.fori_loop(0, nz, one, 0)
        final[part, pl.ds(depth * 2, 2)] = muted[1, part, pl.ds(depth * 2, 2)]

    def final_many(part):
        return many(
            muted.at[1, part],
            final.at[part],
            back_send.at[1, part],
            back_recv.at[1, part],
            slots - 2,
        )

    def tile_many(phase, part):
        where = pl.ds(part * PART, PART)
        return remote(
            sent.at[phase, pl.ds(0, blocks - 1), where],
            got.at[phase, pl.ds(0, blocks - 1), where],
            tile_send.at[phase, part],
            tile_recv.at[phase, part, 0],
            partner,
        )

    def store_plus(part):
        where = slice(part * PART, (part + 1) * PART)
        for slot in range(2):
            value = jnp.concatenate([final[part, 2 * level + slot] for level in range(nz)], axis=0)
            value = valid_rows(value.astype(jnp.float32).T).astype(plus_stage.dtype)
            plus_stage[slot, 0, where] = value[:PART]
            plus_stage[slot, 1, where] = value[PART:]

    for part in range(CHUNKS):
        finish(0, part, left_all, 1.0)
        spread_image(0, part)
        if part > 0:
            back_many(part - 1).wait_recv()
            backward(part - 1)
        freq_many(0, part).wait_recv()
        mute(0, part)
        send_back(part)
    back_many(CHUNKS - 1).wait_recv()
    backward(CHUNKS - 1)
    for part in range(CHUNKS):
        finish(1, part, right_all, -1.0)
        spread_image(1, part)
        if part > 0:
            final_many(part - 1).wait_recv()
            store_plus(part - 1)
            tile_many(1, part - 1).wait_send()
        if part == 0:
            for piece in range(CHUNKS):
                swap(piece).start()
            for piece in range(CHUNKS):
                rows = slice(piece * PART, (piece + 1) * PART)
                own = swap_out[piece, core]
                minus_stage[core, 0, rows] = own[:PART]
                minus_stage[core, 1, rows] = own[PART:]
                swap(piece).wait_recv()
                theirs = swap_in[piece]
                minus_stage[other, 0, rows] = theirs[:PART]
                minus_stage[other, 1, rows] = theirs[PART:]
            minus_copy = local(minus_stage, both_hbm.at[1], out_sem.at[0])
            minus_copy.start()
            for piece in range(CHUNKS):
                tile_many(0, piece).wait_send()
                freq_many(0, piece).wait_send()
                back_many(piece).wait_send()
                swap(piece).wait_send()
            pair.wait_send()
            remote(right_out, right_all.at[core], right_send, right_recv.at[0], partner).wait_send()
            remote(left_out, left_all.at[core], left_send, left_recv.at[0], partner).wait_send()
        freq_many(1, part).wait_recv()
        mute(1, part)
        send_final(part)
    tile_many(1, CHUNKS - 1).wait_send()
    for part in range(CHUNKS):
        freq_many(1, part).wait_send()
    minus_copy.wait()
    final_many(CHUNKS - 1).wait_recv()
    store_plus(CHUNKS - 1)
    plus_copy = local(plus_stage, both_hbm.at[0], out_sem.at[1])
    plus_copy.start()
    for part in range(CHUNKS):
        final_many(part).wait_send()
    plus_copy.wait()


def widen_results(both_hbm, direct_hbm, plus_hbm, minus_hbm, both, direct, wide, in_sem, out_sem):
    ins = [
        pltpu.make_async_copy(both_hbm.at[1], both.at[1], in_sem.at[0]),
        pltpu.make_async_copy(both_hbm.at[0], both.at[0], in_sem.at[1]),
        pltpu.make_async_copy(direct_hbm, direct, in_sem.at[2]),
    ]
    outs = [
        pltpu.make_async_copy(wide.at[1], minus_hbm, out_sem.at[0]),
        pltpu.make_async_copy(wide.at[0], plus_hbm, out_sem.at[1]),
    ]
    for copy in ins:
        copy.start()
    ins[0].wait()
    wide[1] = both[1].astype(jnp.float32)
    outs[0].start()
    ins[1].wait()
    ins[2].wait()
    wide[0] = direct[...] + both[0].astype(jnp.float32)
    outs[1].start()
    for copy in outs:
        copy.wait()


def shards(dims, left_factor, right_factor, tile_ranks, freq_order, mute_window, direct_wave):
    ny, nx, nz, samples_count = dims
    blocks = ny * nx
    slots = 2 * nz
    rows_each = ROWS // nz
    bf16, f32 = jnp.bfloat16, jnp.float32
    dma = pltpu.SemaphoreType.DMA
    turned = jnp.transpose(direct_wave, (0, 1, 3, 2))
    factor = (2, blocks, ROWS, LANES)
    tiles = (blocks, FOCAL, LANES)
    pieces = (2, CHUNKS, slots, rows_each, LANES)
    stage = (2, 2, FOCAL, ROWS)
    each = (2, CHUNKS)
    scratch = [
        pltpu.VMEM((4, ROWS, blocks, LANES), bf16),
        pltpu.VMEM((ROWS * PITCH, LANES), f32),
        pltpu.VMEM(factor, bf16),
        pltpu.VMEM(factor, bf16),
        pltpu.VMEM(factor[1:], bf16),
        pltpu.VMEM(factor[1:], bf16),
        pltpu.VMEM(stage, f32),
        pltpu.VMEM(mute_window.shape, jnp.int32),
        pltpu.VMEM((CHUNKS, rows_each, LANES), jnp.int32),
        pltpu.SMEM(tile_ranks.shape, jnp.int32),
        pltpu.SMEM(freq_order.shape, jnp.int32),
        pltpu.VMEM((2, LANES, ROWS), bf16),
        pltpu.VMEM((LANES, ROWS), bf16),
        pltpu.VMEM(tiles, bf16),
        pltpu.VMEM((2,) + tiles, bf16),
        pltpu.VMEM((2,) + tiles, bf16),
        pltpu.VMEM((2, ROWS, LANES), f32),
        pltpu.VMEM(pieces, bf16),
        pltpu.VMEM(pieces, bf16),
        pltpu.VMEM((slots, samples_count // CHUNKS, LANES), f32),
        pltpu.VMEM((samples_count // CHUNKS, rows_each, LANES), f32),
        pltpu.VMEM(pieces, bf16),
        pltpu.VMEM(pieces[1:], bf16),
        pltpu.VMEM((CHUNKS, 2, 2 * PART, ROWS), bf16),
        pltpu.VMEM((CHUNKS, 2 * PART, ROWS), bf16),
        pltpu.VMEM(pieces[1:], bf16),
        pltpu.VMEM(stage, bf16),
        pltpu.VMEM(stage, bf16),
        dma((4,)),
        dma((4,)),
        dma((2,)),
        dma,
        dma,
        dma((CHUNKS,)),
        dma((CHUNKS,)),
        dma,
        dma((ny,)),
        dma,
        dma((ny,)),
        dma(each),
        dma(each + (blocks,)),
        dma(each),
        dma(each),
        dma(each),
        dma(each),
    ]
    out = jax.ShapeDtypeStruct((2,) + stage, bf16)
    both = pl.pallas_call(
        functools.partial(kernel, dims),
        out_shape=out,
        in_specs=[pl.BlockSpec(memory_space=pltpu.HBM)] * 6,
        out_specs=pl.BlockSpec(memory_space=pl.ANY),
        scratch_shapes=scratch,
        compiler_params=pltpu.CompilerParams(
            collective_id=0, has_side_effects=True, vmem_limit_bytes=66000000
        ),
        name="focusing",
    )(right_factor, left_factor, tile_ranks, freq_order, mute_window, turned)
    wide = jax.ShapeDtypeStruct(stage, f32)
    plus, minus = pl.pallas_call(
        widen_results,
        out_shape=(wide, wide),
        in_specs=[pl.BlockSpec(memory_space=pl.ANY)] * 2,
        out_specs=(pl.BlockSpec(memory_space=pl.ANY),) * 2,
        scratch_shapes=[
            pltpu.VMEM((2,) + stage, bf16),
            pltpu.VMEM(stage, f32),
            pltpu.VMEM((2,) + stage, f32),
            dma((3,)),
            dma((2,)),
        ],
        compiler_params=pltpu.CompilerParams(vmem_limit_bytes=66000000),
        name="widen",
    )(both, turned)
    return jnp.transpose(plus, (0, 1, 3, 2)), jnp.transpose(minus, (0, 1, 3, 2))


def solution(mesh):
    nz = mesh.shape["freq"]
    ny, nx = GRID[mesh.shape["tile"]]
    dims = (ny, nx, nz, 4 * nz)
    return jax.shard_map(
        functools.partial(shards, dims),
        mesh=mesh,
        in_specs=(
            P("freq", "tile", None, None),
            P("freq", "tile", None, None),
            P("freq", None, None),
            P(),
            P(("tile", "freq"), None),
            P("freq", None, "tile", None),
        ),
        out_specs=(P("freq", None, "tile", None), P("freq", None, "tile", None)),
        check_vma=False,
    )
```
